8 devices in a mesh: data: 8 (over z, y, x, core).
Axes of the slice: x: 2, y: 2, z: 1, core: 2. Of those that a mesh axis runs over, the one named last changes fastest.
Arguments:
- tok_ids: int32 [32768], P('data')
- grad_out: bfloat16 [32768, 256], P('data')
- n_real: int32 [8], P('data')
- embed_table: bfloat16 [30522, 256], replicated
- w_in: bfloat16 [256, 1024], replicated
- w_out: bfloat16 [1024, 256], replicated
Outputs:
- output 1: float32 [30522, 256], replicated
- output 2: float32 [256, 1024], replicated
- output 3: float32 [1024, 256], replicated
All inputs are finite; a program needn't handle non-finite values.
Results may differ from the reference program's by a relative error of at most 0.00851241.
Values are sent between devices in bfloat16 or wider.
A program may use at most 1 GiB of HBM per device.

```python
import math
import jax
import jax.numpy as jnp
from jax import lax

NUM_DEV = 8
TOKENS = 4096
VOCAB = 30522
DIM = 256
FFN = 1024

UNIQ_IDS = TOKENS // 4
SHARED_IDS = UNIQ_IDS // 2
GELU_A = 0.044715
GELU_C = math.sqrt(2.0 / math.pi)


def draw_ids(rng_key):
    k_perm, k_dev = jax.random.split(rng_key)
    vocab_perm = jax.random.permutation(k_perm, VOCAB)
    shared_ids = vocab_perm[:SHARED_IDS]
    other_ids = vocab_perm[SHARED_IDS:]

    def one_device(dev_key):
        k_own, k_order, k_fill = jax.random.split(dev_key, 3)
        own_pick = jax.random.permutation(k_own, VOCAB - SHARED_IDS)[:UNIQ_IDS - SHARED_IDS]
        distinct = jnp.concatenate([shared_ids, other_ids[own_pick]])
        distinct = jax.random.permutation(k_order, distinct)
        filler = distinct[jax.random.randint(k_fill, (TOKENS - UNIQ_IDS,), 0, UNIQ_IDS)]
        return jnp.concatenate([distinct, filler])

    per_dev = jax.vmap(one_device)(jax.random.split(k_dev, NUM_DEV))
    return per_dev.reshape(NUM_DEV * TOKENS).astype(jnp.int32)


def draw_lengths(rng_key):
    k_len, k_pos = jax.random.split(rng_key)
    lengths = jax.random.randint(k_len, (NUM_DEV,), TOKENS // 4, TOKENS + 1)
    dev_order = jax.random.permutation(k_pos, NUM_DEV)
    lengths = lengths.at[dev_order[0]].set(TOKENS).at[dev_order[1]].set(TOKENS // 4)
    return lengths.astype(jnp.int32)


def setup_inputs(seed: int = 0) -> dict:
    root_key = jax.random.key(seed)
    k_ids, k_len, k_dy, k_tab, k_in, k_out = jax.random.split(root_key, 6)
    grad_out = jax.random.normal(k_dy, (NUM_DEV * TOKENS, DIM), jnp.float32) * NUM_DEV ** -0.5
    embed_table = jax.random.normal(k_tab, (VOCAB, DIM), jnp.float32)
    w_in = jax.random.normal(k_in, (DIM, FFN), jnp.float32) * DIM ** -0.5
    w_out = jax.random.normal(k_out, (FFN, DIM), jnp.float32) * FFN ** -0.5
    return {
        'tok_ids': draw_ids(k_ids),
        'grad_out': grad_out.astype(jnp.bfloat16),
        'n_real': draw_lengths(k_len),
        'embed_table': embed_table.astype(jnp.bfloat16),
        'w_in': w_in.astype(jnp.bfloat16),
        'w_out': w_out.astype(jnp.bfloat16),
    }


def gelu_and_slope(pre_act):
    z_val = pre_act.astype(jnp.float32)
    tanh_val = jnp.tanh(GELU_C * (z_val + GELU_A * z_val * z_val * z_val))
    act_val = 0.5 * z_val * (1.0 + tanh_val)
    slope_val = 0.5 * (1.0 + tanh_val) + 0.5 * z_val * (1.0 - tanh_val * tanh_val) * GELU_C * (1.0 + 3.0 * GELU_A * z_val * z_val)
    return act_val, slope_val


def device_grads(ids_one, dy_one, n_one, embed_table, w_in, w_out):
    x_rows = jnp.take(embed_table, ids_one, axis=0)
    keep_mask = (jnp.arange(ids_one.shape[0]) < n_one)[:, None]
    dy_kept = jnp.where(keep_mask, dy_one, jnp.zeros_like(dy_one))
    pre_act = jnp.dot(x_rows, w_in, preferred_element_type=jnp.float32).astype(jnp.bfloat16)
    act_val, slope_val = gelu_and_slope(pre_act)
    act_bf16 = act_val.astype(jnp.bfloat16)
    part_out = jnp.dot(act_bf16.T, dy_kept, preferred_element_type=jnp.float32)
    grad_act = jnp.dot(dy_kept, w_out.T, preferred_element_type=jnp.float32).astype(jnp.bfloat16)
    grad_pre = (grad_act.astype(jnp.float32) * slope_val).astype(jnp.bfloat16)
    part_in = jnp.dot(x_rows.T, grad_pre, preferred_element_type=jnp.float32)
    grad_x = (dy_kept.astype(jnp.float32) + jnp.dot(grad_pre, w_in.T, preferred_element_type=jnp.float32)).astype(jnp.bfloat16)
    return grad_x, part_in, part_out


def reference(tok_ids, grad_out, n_real, embed_table, w_in, w_out):
    ids_dev = tok_ids.reshape(NUM_DEV, TOKENS)
    dy_dev = grad_out.reshape(NUM_DEV, TOKENS, DIM)

    def body(carry_acc, per_dev):
        acc_in, acc_out = carry_acc
        ids_one, dy_one, n_one = per_dev
        grad_x, part_in, part_out = device_grads(ids_one, dy_one, n_one, embed_table, w_in, w_out)
        return (acc_in + part_in, acc_out + part_out), grad_x

    init_acc = (jnp.zeros((DIM, FFN), jnp.float32), jnp.zeros((FFN, DIM), jnp.float32))
    (grad_w_in, grad_w_out), grad_x = lax.scan(body, init_acc, (ids_dev, dy_dev, n_real))
    flat_rows = grad_x.reshape(NUM_DEV * TOKENS, DIM).astype(jnp.float32)
    grad_table = jax.ops.segment_sum(flat_rows, tok_ids, num_segments=VOCAB)
    return grad_table, grad_w_in, grad_w_out
```

```python
import functools
import math

import jax
import jax.numpy as jnp
from jax import lax
from jax.experimental import pallas as pl
from jax.experimental.pallas import tpu as pltpu
from jax.sharding import PartitionSpec as P

GELU_A = 0.044715
GELU_C = math.sqrt(2.0 / math.pi)

NDEV = 8
TOK = 4096
VOCAB = 30522
DIM = 256
FFN = 1024
UNIQ = 1024
HI = 128
LO = 256
STEP_TOK = 512
CHUNK_HI = 16
CHUNK = CHUNK_HI * LO
NCHUNK = -(-VOCAB // CHUNK)
LAST = VOCAB - (NCHUNK - 1) * CHUNK
BATCH = 16
META = UNIQ + HI

F32 = jnp.float32
BF16 = jnp.bfloat16
VMEM_LIMIT = 62 * 1024 * 1024


def dot(a, b, ca, cb):
    return lax.dot_general(a, b, (((ca,), (cb,)), ((), ())), preferred_element_type=F32)


def iota(shape, axis):
    return lax.broadcasted_iota(jnp.int32, shape, axis)


def dedup_kernel(n_ref, ids_ref, dy_ref, meta_ref, msum_ref):
    ids = ids_ref[...]
    ohi = (iota((HI, TOK), 0) == (ids >> 8)).astype(BF16)
    olo = (iota((LO, TOK), 0) == (ids & 255)).astype(BF16)
    present = (dot(ohi, olo, 1, 1) > 0.5).astype(BF16)
    upper = (iota((LO, LO), 0) < iota((LO, LO), 1)).astype(BF16)
    before = dot(present, upper, 1, 0)
    total = dot(present, jnp.ones((LO, UNIQ), BF16), 1, 0)
    lower = (iota((HI, HI), 1) < iota((HI, HI), 0)).astype(BF16)
    offset = dot(lower, total.astype(BF16), 1, 0)
    rank = before + offset[:, :LO]
    rank_a = jnp.floor(rank * (1.0 / 32.0))
    rank_b = (rank - 32.0 * rank_a).astype(BF16)
    rank_a = rank_a.astype(BF16)

    lane = iota((HI, UNIQ), 1).astype(F32)
    hi_of = jnp.sum(((offset + total) <= lane).astype(F32), axis=0, keepdims=True)
    hot = iota((HI, UNIQ), 0).astype(F32) == hi_of
    k_of = lane[:1] - jnp.sum(jnp.where(hot, offset, 0.0), axis=0, keepdims=True)
    upto = (before + present.astype(F32)).astype(BF16)
    row_of = dot(upto, hot.astype(BF16), 0, 0)
    lo_of = jnp.sum((row_of <= k_of).astype(F32), axis=0, keepdims=True)
    meta_ref[:, :UNIQ] = (hi_of * 256.0 + lo_of).astype(jnp.int32)
    eye = iota((HI, HI), 0) == iota((HI, HI), 1)
    meta_ref[:, UNIQ:] = jnp.sum(jnp.where(eye, offset[:, :HI], 0.0), axis=0, keepdims=True).astype(jnp.int32)

    kept = n_ref[0]
    for b in range(TOK // STEP_TOK):
        cols = slice(b * STEP_TOK, (b + 1) * STEP_TOK)
        mine = ohi[:, cols]
        pos = 32.0 * dot(rank_a, mine, 0, 0) + dot(rank_b, mine, 0, 0)
        slot = jnp.sum(pos * olo[:, cols].astype(F32), axis=0, keepdims=True)
        tok = iota((1, STEP_TOK), 1) + b * STEP_TOK
        slot = jnp.where(tok < kept, slot.astype(jnp.int32), -1)
        pick = (iota((UNIQ, STEP_TOK), 0) == slot).astype(BF16)
        part = dot(pick, dy_ref[cols, :], 1, 0)
        if b == 0:
            msum_ref[...] = part
        else:
            msum_ref[...] += part


def dedup(n_real, ids, dy):
    return pl.pallas_call(
        dedup_kernel,
        out_shape=(jax.ShapeDtypeStruct((1, META), jnp.int32), jax.ShapeDtypeStruct((UNIQ, DIM), F32)),
        in_specs=[pl.BlockSpec(memory_space=pltpu.SMEM), pl.BlockSpec(memory_space=pltpu.VMEM), pl.BlockSpec(memory_space=pltpu.VMEM)],
        out_specs=(pl.BlockSpec(memory_space=pltpu.VMEM), pl.BlockSpec(memory_space=pltpu.VMEM)),
        compiler_params=pltpu.CompilerParams(vmem_limit_bytes=VMEM_LIMIT),
        name="dedup",
    )(n_real, ids, dy)


def grads_kernel(x_ref, m_ref, w1_ref, w2_ref, dx_ref, dw1_ref, dw2_ref):
    first = pl.program_id(0) == 0
    x = x_ref[...]
    m = m_ref[...]
    m_hi = m.astype(BF16)
    m_lo = (m - m_hi.astype(F32)).astype(BF16)
    z = dot(x, w1_ref[...], 1, 0).astype(BF16).astype(F32)
    t = jnp.tanh(GELU_C * (z + GELU_A * z * z * z))
    h = (0.5 * z * (1.0 + t)).astype(BF16)
    slope = 0.5 * (1.0 + t) + 0.5 * z * (1.0 - t * t) * GELU_C * (1.0 + 3.0 * GELU_A * z * z)
    dh = (dot(m_hi, w2_ref[...], 1, 1) + dot(m_lo, w2_ref[...], 1, 1)).astype(BF16).astype(F32)
    dz = (dh * slope).astype(BF16)
    dx_ref[...] = m + dot(dz, w1_ref[...], 1, 1)
    dw1 = dot(x, dz, 0, 0)
    dw2 = dot(h, m_hi, 0, 0) + dot(h, m_lo, 0, 0)

    @pl.when(first)
    def _():
        dw1_ref[...] = dw1
        dw2_ref[...] = dw2

    @pl.when(jnp.logical_not(first))
    def _():
        dw1_ref[...] += dw1
        dw2_ref[...] += dw2


def grads(x, m, w1, w2):
    rows = 256
    return pl.pallas_call(
        grads_kernel,
        grid=(UNIQ // rows,),
        out_shape=(jax.ShapeDtypeStruct((UNIQ, DIM), F32), jax.ShapeDtypeStruct((DIM, FFN), F32), jax.ShapeDtypeStruct((FFN, DIM), F32)),
        in_specs=[pl.BlockSpec((rows, DIM), lambda i: (i, 0)), pl.BlockSpec((rows, DIM), lambda i: (i, 0)),
                  pl.BlockSpec((DIM, FFN), lambda i: (0, 0)), pl.BlockSpec((FFN, DIM), lambda i: (0, 0))],
        out_specs=(pl.BlockSpec((rows, DIM), lambda i: (i, 0)), pl.BlockSpec((DIM, FFN), lambda i: (0, 0)), pl.BlockSpec((FFN, DIM), lambda i: (0, 0))),
        compiler_params=pltpu.CompilerParams(vmem_limit_bytes=VMEM_LIMIT, dimension_semantics=("arbitrary",)),
        name="grads",
    )(x, m, w1, w2)


def table_kernel(meta_ref, rows_hbm, out_hbm, rows, acc, in_sem, out_sem):
    def in_copy(d, half):
        part = pl.ds(d * UNIQ, UNIQ)
        return pltpu.make_async_copy(rows_hbm.at[part, pl.ds(half * 128, 128)], rows.at[half, part], in_sem.at[d, half])

    for d in range(NDEV):
        for half in range(2):
            in_copy(d, half).start()

    def out_copy(c, slot, half):
        size = CHUNK if c < NCHUNK - 1 else LAST
        return pltpu.make_async_copy(acc.at[slot, half, pl.ds(0, size)], out_hbm.at[pl.ds(c * CHUNK, size), pl.ds(half * 128, 128)], out_sem.at[slot, half])

    for c in range(NCHUNK):
        slot = c % 2
        if c >= 2:
            for half in range(2):
                out_copy(c - 2, slot, half).wait()
        acc[slot, :, pl.ds(0, CHUNK)] = jnp.zeros((2, CHUNK, 128), F32)
        for d in range(NDEV):
            if c == 0:
                for half in range(2):
                    in_copy(d, half).wait()
            start = meta_ref[d, UNIQ + c * CHUNK_HI]
            end = meta_ref[d, UNIQ + (c + 1) * CHUNK_HI] if (c + 1) * CHUNK_HI < HI else UNIQ

            @pl.loop(start // BATCH, (end + BATCH - 1) // BATCH)
            def _(b):
                base = pl.multiple_of(b * BATCH, BATCH)
                at = []
                for k in range(BATCH):
                    loc = meta_ref[d, base + k] - c * CHUNK
                    at.append(jnp.where((loc >= 0) & (loc < CHUNK), loc, CHUNK))
                sums = []
                for k in range(BATCH):
                    for half in range(2):
                        sums.append(acc[slot, half, pl.ds(at[k], 1), :] + rows[half, pl.ds(d * UNIQ + base + k, 1), :])
                for k in range(BATCH):
                    for half in range(2):
                        acc[slot, half, pl.ds(at[k], 1), :] = sums[2 * k + half]
        for half in range(2):
            out_copy(c, slot, half).start()
    for c in range(max(0, NCHUNK - 2), NCHUNK):
        for half in range(2):
            out_copy(c, c % 2, half).wait()


def table(meta, rows):
    return pl.pallas_call(
        table_kernel,
        grid_spec=pltpu.PrefetchScalarGridSpec(
            num_scalar_prefetch=1, grid=(1,),
            in_specs=[pl.BlockSpec(memory_space=pl.ANY)], out_specs=pl.BlockSpec(memory_space=pl.ANY),
            scratch_shapes=[pltpu.VMEM((2, NDEV * UNIQ, 128), F32), pltpu.VMEM((2, 2, CHUNK + 8, 128), F32),
                            pltpu.SemaphoreType.DMA((NDEV, 2)), pltpu.SemaphoreType.DMA((2, 2))]),
        out_shape=jax.ShapeDtypeStruct((VOCAB, DIM), F32),
        compiler_params=pltpu.CompilerParams(vmem_limit_bytes=VMEM_LIMIT),
        name="table",
    )(meta, rows)


def solution(mesh):
    def per_device(tok_ids, grad_out, n_real, embed_table, w_in, w_out):
        meta, msum = dedup(n_real, tok_ids.reshape(1, TOK), grad_out)
        x = jnp.take(embed_table, meta[0, :UNIQ], axis=0, mode='clip')
        dx, part_in, part_out = grads(x, msum, w_in, w_out)
        grad_w_in = lax.psum(part_in, 'data')
        grad_w_out = lax.psum(part_out, 'data')
        all_meta = lax.all_gather(meta, 'data', tiled=True)
        all_rows = lax.all_gather(dx, 'data', tiled=True)
        return table(all_meta, all_rows), grad_w_in, grad_w_out

    return jax.shard_map(per_device, mesh=mesh, in_specs=(P('data'), P('data', None), P('data'), P(), P(), P()), out_specs=(P(), P(), P()), check_vma=False)
```

```python
import functools
import math

import jax
import jax.numpy as jnp
from jax import lax
from jax.experimental import pallas as pl
from jax.experimental.pallas import tpu as pltpu
from jax.sharding import PartitionSpec as P

GELU_A = 0.044715
GELU_C = math.sqrt(2.0 / math.pi)

NDEV = 8
TOK = 4096
VOCAB = 30522
DIM = 256
FFN = 1024
UNIQ = 1024
HI = 128
LO = 256
STEP_TOK = 512
CHUNK_HI = 16
CHUNK = CHUNK_HI * LO
NCHUNK = -(-VOCAB // CHUNK)
LAST = VOCAB - (NCHUNK - 1) * CHUNK
BATCH = 8
PADDED = 30528
ZERO = 192
META = UNIQ + HI

F32 = jnp.float32
BF16 = jnp.bfloat16
VMEM_LIMIT = 62 * 1024 * 1024


def dot(a, b, ca, cb):
    return lax.dot_general(a, b, (((ca,), (cb,)), ((), ())), preferred_element_type=F32)


def iota(shape, axis):
    return lax.broadcasted_iota(jnp.int32, shape, axis)


def dedup_kernel(n_ref, ids_ref, dy_ref, meta_ref, msum_ref):
    ids = ids_ref[...]
    ohi = (iota((HI, TOK), 0) == (ids >> 8)).astype(BF16)
    olo = (iota((LO, TOK), 0) == (ids & 255)).astype(BF16)
    present = (dot(ohi, olo, 1, 1) > 0.5).astype(BF16)
    upper = (iota((LO, LO), 0) < iota((LO, LO), 1)).astype(BF16)
    before = dot(present, upper, 1, 0)
    total = dot(present, jnp.ones((LO, UNIQ), BF16), 1, 0)
    lower = (iota((HI, HI), 1) < iota((HI, HI), 0)).astype(BF16)
    offset = dot(lower, total.astype(BF16), 1, 0)
    rank = before + offset[:, :LO]
    rank_a = jnp.floor(rank * (1.0 / 32.0))
    rank_b = (rank - 32.0 * rank_a).astype(BF16)
    rank_a = rank_a.astype(BF16)

    lane = iota((HI, UNIQ), 1).astype(F32)
    hi_of = jnp.sum(((offset + total) <= lane).astype(F32), axis=0, keepdims=True)
    hot = iota((HI, UNIQ), 0).astype(F32) == hi_of
    k_of = lane[:1] - jnp.sum(jnp.where(hot, offset, 0.0), axis=0, keepdims=True)
    upto = (before + present.astype(F32)).astype(BF16)
    row_of = dot(upto, hot.astype(BF16), 0, 0)
    lo_of = jnp.sum((row_of <= k_of).astype(F32), axis=0, keepdims=True)
    meta_ref[:, :UNIQ] = (hi_of * 256.0 + lo_of).astype(jnp.int32)
    eye = iota((HI, HI), 0) == iota((HI, HI), 1)
    meta_ref[:, UNIQ:] = jnp.sum(jnp.where(eye, offset[:, :HI], 0.0), axis=0, keepdims=True).astype(jnp.int32)

    kept = n_ref[0]
    for b in range(TOK // STEP_TOK):
        cols = slice(b * STEP_TOK, (b + 1) * STEP_TOK)
        mine = ohi[:, cols]
        pos = 32.0 * dot(rank_a, mine, 0, 0) + dot(rank_b, mine, 0, 0)
        slot = jnp.sum(pos * olo[:, cols].astype(F32), axis=0, keepdims=True)
        tok = iota((1, STEP_TOK), 1) + b * STEP_TOK
        slot = jnp.where(tok < kept, slot.astype(jnp.int32), -1)
        pick = (iota((UNIQ, STEP_TOK), 0) == slot).astype(BF16)
        part = dot(pick, dy_ref[cols, :], 1, 0)
        if b == 0:
            msum_ref[...] = part
        else:
            msum_ref[...] += part


def dedup(n_real, ids, dy):
    return pl.pallas_call(
        dedup_kernel,
        out_shape=(jax.ShapeDtypeStruct((1, META), jnp.int32), jax.ShapeDtypeStruct((UNIQ, DIM), F32)),
        in_specs=[pl.BlockSpec(memory_space=pltpu.SMEM), pl.BlockSpec(memory_space=pltpu.VMEM), pl.BlockSpec(memory_space=pltpu.VMEM)],
        out_specs=(pl.BlockSpec(memory_space=pltpu.VMEM), pl.BlockSpec(memory_space=pltpu.VMEM)),
        compiler_params=pltpu.CompilerParams(vmem_limit_bytes=VMEM_LIMIT),
        name="dedup",
    )(n_real, ids, dy)


def grads_kernel(x_ref, m_ref, w1_ref, w2_ref, dx_ref, dw1_ref, dw2_ref):
    first = pl.program_id(0) == 0
    x = x_ref[...]
    m = m_ref[...]
    m_hi = m.astype(BF16)
    m_lo = (m - m_hi.astype(F32)).astype(BF16)
    z = dot(x, w1_ref[...], 1, 0).astype(BF16).astype(F32)
    t = jnp.tanh(GELU_C * (z + GELU_A * z * z * z))
    h = (0.5 * z * (1.0 + t)).astype(BF16)
    slope = 0.5 * (1.0 + t) + 0.5 * z * (1.0 - t * t) * GELU_C * (1.0 + 3.0 * GELU_A * z * z)
    dh = (dot(m_hi, w2_ref[...], 1, 1) + dot(m_lo, w2_ref[...], 1, 1)).astype(BF16).astype(F32)
    dz = (dh * slope).astype(BF16)
    dx_ref[...] = m + dot(dz, w1_ref[...], 1, 1)
    dw1 = dot(x, dz, 0, 0)
    dw2 = dot(h, m_hi, 0, 0) + dot(h, m_lo, 0, 0)

    @pl.when(first)
    def _():
        dw1_ref[...] = dw1
        dw2_ref[...] = dw2

    @pl.when(jnp.logical_not(first))
    def _():
        dw1_ref[...] += dw1
        dw2_ref[...] += dw2


def grads(x, m, w1, w2):
    rows = 256
    return pl.pallas_call(
        grads_kernel,
        grid=(UNIQ // rows,),
        out_shape=(jax.ShapeDtypeStruct((UNIQ, DIM), F32), jax.ShapeDtypeStruct((DIM, FFN), F32), jax.ShapeDtypeStruct((FFN, DIM), F32)),
        in_specs=[pl.BlockSpec((rows, DIM), lambda i: (i, 0)), pl.BlockSpec((rows, DIM), lambda i: (i, 0)),
                  pl.BlockSpec((DIM, FFN), lambda i: (0, 0)), pl.BlockSpec((FFN, DIM), lambda i: (0, 0))],
        out_specs=(pl.BlockSpec((rows, DIM), lambda i: (i, 0)), pl.BlockSpec((DIM, FFN), lambda i: (0, 0)), pl.BlockSpec((FFN, DIM), lambda i: (0, 0))),
        compiler_params=pltpu.CompilerParams(vmem_limit_bytes=VMEM_LIMIT, dimension_semantics=("arbitrary",)),
        name="grads",
    )(x, m, w1, w2)


def table_kernel(uid_ref, off_ref, rows_hbm, out_hbm, rows, acc, in_sem, out_sem):
    def in_copy(d, half):
        part = pl.ds(d * UNIQ, UNIQ)
        return pltpu.make_async_copy(rows_hbm.at[part, pl.ds(half * 128, 128)], rows.at[half, part], in_sem.at[d, half])

    def out_copy(c, half):
        part = pl.ds(c * CHUNK, CHUNK if c < NCHUNK - 1 else LAST)
        return pltpu.make_async_copy(acc.at[half, part], out_hbm.at[part, pl.ds(half * 128, 128)], out_sem.at[c, half])

    for d in range(NDEV):
        for half in range(2):
            in_copy(d, half).start()

    @pl.loop(0, PADDED // ZERO)
    def _(i):
        part = pl.ds(pl.multiple_of(i * ZERO, ZERO), ZERO)
        for half in range(2):
            acc[half, part] = jnp.zeros((ZERO, 128), F32)

    for d in range(NDEV):
        for half in range(2):
            in_copy(d, half).wait()

    for c in range(NCHUNK):
        for d in range(NDEV):
            first = (off_ref[d * HI + c * CHUNK_HI] + BATCH - 1) // BATCH
            last = (off_ref[d * HI + (c + 1) * CHUNK_HI] + BATCH - 1) // BATCH if c < NCHUNK - 1 else UNIQ // BATCH

            def fetch(b):
                base = pl.multiple_of(d * UNIQ + b * BATCH, BATCH)
                sums = []
                for half in range(2):
                    for k in range(BATCH):
                        sums.append(acc[half, pl.ds(uid_ref[base + k], 1), :] + rows[half, pl.ds(base + k, 1), :])
                return sums

            def put(b, sums):
                base = pl.multiple_of(d * UNIQ + b * BATCH, BATCH)
                for half in range(2):
                    for k in range(BATCH):
                        acc[half, pl.ds(uid_ref[base + k], 1), :] = sums[half * BATCH + k]

            def step(b, sums):
                ahead = fetch(b)
                put(b - 1, sums)
                return ahead

            @pl.when(last > first)
            def _():
                sums = lax.fori_loop(first + 1, last, step, fetch(first))
                put(last - 1, sums)

        for half in range(2):
            out_copy(c, half).start()
    for c in range(NCHUNK):
        for half in range(2):
            out_copy(c, half).wait()


def table(meta, rows):
    return pl.pallas_call(
        table_kernel,
        grid_spec=pltpu.PrefetchScalarGridSpec(
            num_scalar_prefetch=2, grid=(1,),
            in_specs=[pl.BlockSpec(memory_space=pl.ANY)], out_specs=pl.BlockSpec(memory_space=pl.ANY),
            scratch_shapes=[pltpu.VMEM((2, NDEV * UNIQ, 128), F32), pltpu.VMEM((2, PADDED, 128), F32),
                            pltpu.SemaphoreType.DMA((NDEV, 2)), pltpu.SemaphoreType.DMA((NCHUNK, 2))]),
        out_shape=jax.ShapeDtypeStruct((VOCAB, DIM), F32),
        compiler_params=pltpu.CompilerParams(vmem_limit_bytes=VMEM_LIMIT),
        name="table",
    )(meta[:, :UNIQ].reshape(-1), meta[:, UNIQ:].reshape(-1), rows)


def solution(mesh):
    def per_device(tok_ids, grad_out, n_real, embed_table, w_in, w_out):
        meta, msum = dedup(n_real, tok_ids.reshape(1, TOK), grad_out)
        x = jnp.take(embed_table, meta[0, :UNIQ], axis=0, mode='clip')
        dx, part_in, part_out = grads(x, msum, w_in, w_out)
        grad_w_in = lax.psum(part_in, 'data')
        grad_w_out = lax.psum(part_out, 'data')
        all_meta = lax.all_gather(meta, 'data', tiled=True)
        all_rows = lax.all_gather(dx, 'data', tiled=True)
        return table(all_meta, all_rows), grad_w_in, grad_w_out

    return jax.shard_map(per_device, mesh=mesh, in_specs=(P('data'), P('data', None), P('data'), P(), P(), P()), out_specs=(P(), P(), P()), check_vma=False)
```

```python
import functools
import math

import jax
import jax.numpy as jnp
from jax import lax
from jax.experimental import pallas as pl
from jax.experimental.pallas import tpu as pltpu
from jax.sharding import PartitionSpec as P

GELU_A = 0.044715
GELU_C = math.sqrt(2.0 / math.pi)

NDEV = 8
TOK = 4096
VOCAB = 30522
DIM = 256
FFN = 1024
UNIQ = 1024
HI = 128
LO = 256
STEP_TOK = 512
CHUNK_HI = 16
CHUNK = CHUNK_HI * LO
NCHUNK = -(-VOCAB // CHUNK)
LAST = VOCAB - (NCHUNK - 1) * CHUNK
BATCH = 8
PADDED = 30528
ZERO = 192
PIECES = 4
PIECE = UNIQ // PIECES
QROWS = DIM // 4
META = UNIQ + HI

F32 = jnp.float32
BF16 = jnp.bfloat16
VMEM_LIMIT = 62 * 1024 * 1024


def dot(a, b, ca, cb):
    return lax.dot_general(a, b, (((ca,), (cb,)), ((), ())), preferred_element_type=F32)


def iota(shape, axis):
    return lax.broadcasted_iota(jnp.int32, shape, axis)


def dedup_kernel(n_ref, ids_ref, dy_ref, meta_ref, msum_ref):
    ids = ids_ref[...]
    ohi = (iota((HI, TOK), 0) == (ids >> 8)).astype(BF16)
    olo = (iota((LO, TOK), 0) == (ids & 255)).astype(BF16)
    present = (dot(ohi, olo, 1, 1) > 0.5).astype(BF16)
    upper = (iota((LO, LO), 0) < iota((LO, LO), 1)).astype(BF16)
    before = dot(present, upper, 1, 0)
    total = dot(present, jnp.ones((LO, UNIQ), BF16), 1, 0)
    lower = (iota((HI, HI), 1) < iota((HI, HI), 0)).astype(BF16)
    offset = dot(lower, total.astype(BF16), 1, 0)
    rank = before + offset[:, :LO]
    rank_a = jnp.floor(rank * (1.0 / 32.0))
    rank_b = (rank - 32.0 * rank_a).astype(BF16)
    rank_a = rank_a.astype(BF16)

    lane = iota((HI, UNIQ), 1).astype(F32)
    hi_of = jnp.sum(((offset + total) <= lane).astype(F32), axis=0, keepdims=True)
    hot = iota((HI, UNIQ), 0).astype(F32) == hi_of
    k_of = lane[:1] - jnp.sum(jnp.where(hot, offset, 0.0), axis=0, keepdims=True)
    upto = (before + present.astype(F32)).astype(BF16)
    row_of = dot(upto, hot.astype(BF16), 0, 0)
    lo_of = jnp.sum((row_of <= k_of).astype(F32), axis=0, keepdims=True)
    meta_ref[:, :UNIQ] = (hi_of * 256.0 + lo_of).astype(jnp.int32)
    eye = iota((HI, HI), 0) == iota((HI, HI), 1)
    meta_ref[:, UNIQ:] = jnp.sum(jnp.where(eye, offset[:, :HI], 0.0), axis=0, keepdims=True).astype(jnp.int32)

    kept = n_ref[0]
    for b in range(TOK // STEP_TOK):
        cols = slice(b * STEP_TOK, (b + 1) * STEP_TOK)
        mine = ohi[:, cols]
        pos = 32.0 * dot(rank_a, mine, 0, 0) + dot(rank_b, mine, 0, 0)
        slot = jnp.sum(pos * olo[:, cols].astype(F32), axis=0, keepdims=True)
        tok = iota((1, STEP_TOK), 1) + b * STEP_TOK
        slot = jnp.where(tok < kept, slot.astype(jnp.int32), -1)
        pick = (iota((UNIQ, STEP_TOK), 0) == slot).astype(BF16)
        part = dot(pick, dy_ref[cols, :], 1, 0)
        if b == 0:
            msum_ref[...] = part
        else:
            msum_ref[...] += part


def dedup(n_real, ids, dy):
    return pl.pallas_call(
        dedup_kernel,
        out_shape=(jax.ShapeDtypeStruct((1, META), jnp.int32), jax.ShapeDtypeStruct((UNIQ, DIM), F32)),
        in_specs=[pl.BlockSpec(memory_space=pltpu.SMEM), pl.BlockSpec(memory_space=pltpu.VMEM), pl.BlockSpec(memory_space=pltpu.VMEM)],
        out_specs=(pl.BlockSpec(memory_space=pltpu.VMEM), pl.BlockSpec(memory_space=pltpu.VMEM)),
        compiler_params=pltpu.CompilerParams(vmem_limit_bytes=VMEM_LIMIT),
        name="dedup",
    )(n_real, ids, dy)


def exchange_kernel(x_ref, m_ref, w1_ref, w2_ref, meta_ref, rows_ref, meta_out, red_ref,
                    dx, part, pin, chip, rs, fin, row_send, row_recv, meta_send, meta_recv, w_send, w_recv, own_sem):
    me = lax.axis_index('data')
    core, px, py = me % 2, (me // 2) % 2, me // 4

    def dev(r):
        return me + (r & 1) * (1 - 2 * core) + ((r >> 1) & 1) * (2 - 4 * px) + ((r >> 2) & 1) * (4 - 8 * py)

    def remote(src, dst, send, recv, r):
        return pltpu.make_async_remote_copy(src_ref=src, dst_ref=dst, send_sem=send, recv_sem=recv, device_id=(dev(r),), device_id_type=pl.DeviceIdType.MESH)

    barrier = pltpu.get_barrier_semaphore()
    for r in (1, 2, 4, 6):
        pl.semaphore_signal(barrier, inc=1, device_id=(dev(r),), device_id_type=pl.DeviceIdType.MESH)
    pl.semaphore_wait(barrier, 4)

    sent = []

    def rows_at(r, k):
        return rows_ref.at[pl.ds(pl.multiple_of(dev(r) * UNIQ + k * PIECE, PIECE), PIECE)]

    def send_rows(block, k, to, src=None):
        copy = remote(rows_at(block, k) if src is None else src, rows_at(block, k), row_send.at[block, k, to // 2], row_recv.at[block ^ to, k], to)
        copy.start()
        sent.append(copy)

    def got_rows(block, k):
        remote(rows_at(block, k), rows_at(block, k), row_send.at[block, k, 0], row_recv.at[block, k], 1).wait_recv()

    def send_meta(block, to):
        src = meta_ref if block == 0 else meta_out.at[dev(block)]
        copy = remote(src, meta_out.at[dev(block)], meta_send.at[block, to // 2], meta_recv.at[block ^ to], to)
        copy.start()
        sent.append(copy)

    def got_meta(block):
        at = meta_out.at[dev(block)]
        remote(at, at, meta_send.at[block, 0], meta_recv.at[block], 1).wait_recv()

    own = [pltpu.make_async_copy(meta_ref, meta_out.at[me], own_sem.at[PIECES])]
    own[0].start()
    for to in (1, 2, 4, 6):
        send_meta(0, to)

    for k in range(PIECES):
        part_rows = pl.ds(k * PIECE, PIECE)
        x = x_ref[part_rows, :]
        m = m_ref[part_rows, :]
        m_hi = m.astype(BF16)
        m_lo = (m - m_hi.astype(F32)).astype(BF16)
        z = dot(x, w1_ref[...], 1, 0).astype(BF16).astype(F32)
        t = jnp.tanh(GELU_C * (z + GELU_A * z * z * z))
        h = (0.5 * z * (1.0 + t)).astype(BF16)
        slope = 0.5 * (1.0 + t) + 0.5 * z * (1.0 - t * t) * GELU_C * (1.0 + 3.0 * GELU_A * z * z)
        dh = (dot(m_hi, w2_ref[...], 1, 1) + dot(m_lo, w2_ref[...], 1, 1)).astype(BF16).astype(F32)
        dz = (dh * slope).astype(BF16)
        dx[part_rows, :] = m + dot(dz, w1_ref[...], 1, 1)
        dw1 = dot(x, dz, 0, 0)
        dw2 = dot(m_hi, h, 0, 0) + dot(m_lo, h, 0, 0)
        part[0] = dw1 if k == 0 else part[0] + dw1
        part[1] = dw2 if k == 0 else part[1] + dw2
        src = dx.at[part_rows]
        for to in (2, 4, 1):
            send_rows(0, k, to, src)
        copy = pltpu.make_async_copy(src, rows_at(0, k), own_sem.at[k])
        copy.start()
        own.append(copy)

    def w_copy(src, dst, i, to):
        copy = remote(src, dst, w_send.at[i], w_recv.at[i], to)
        copy.start()
        sent.append(copy)

    def quarter(r):
        return pl.ds(pl.multiple_of((dev(r) // 2) * QROWS, QROWS), QROWS)

    w_copy(part.at[1 - core], pin, 0, 1)
    remote(pin, pin, w_send.at[0], w_recv.at[0], 1).wait_recv()
    chip[...] = part[core] + pin[...]
    for i, to in enumerate((2, 4, 6)):
        w_copy(chip.at[quarter(to)], rs.at[i], 1 + i, to)

    for block in (2, 4, 6):
        got_meta(block)
        send_meta(block, 1)

    for k in range(PIECES):
        got_rows(2, k)
        if k < PIECES // 2:
            send_rows(2, k, 4)
        send_rows(2, k, 1)
        got_rows(4, k)
        if k >= PIECES // 2:
            send_rows(4, k, 2)
        send_rows(4, k, 1)

    for i, to in enumerate((2, 4, 6)):
        remote(rs.at[i], rs.at[i], w_send.at[1 + i], w_recv.at[1 + i], to).wait_recv()
    fin[...] = (chip[quarter(0), :] + rs[0]) + (rs[1] + rs[2])

    def red_at(r):
        return red_ref.at[(core + r) % 2, quarter(r)]

    for i, to in enumerate((2, 4, 6)):
        w_copy(fin, red_at(0), 4 + i, to)
    w_copy(fin, red_at(0), 7, 1)
    copy = pltpu.make_async_copy(fin, red_at(0), own_sem.at[PIECES + 1])
    copy.start()
    own.append(copy)

    for k in range(PIECES):
        got_rows(6, k)
        send_rows(6, k, 1)

    for i, block in enumerate((2, 4, 6)):
        remote(red_at(block), red_at(block), w_send.at[4 + i], w_recv.at[4 + i], 1).wait_recv()
        w_copy(red_at(block), red_at(block), 8 + i, 1)

    for block in (1, 3, 5, 7):
        got_meta(block)
        for k in range(PIECES):
            got_rows(block, k)
    for i, block in enumerate((1, 3, 5, 7)):
        remote(red_at(block), red_at(block), w_send.at[7 + i], w_recv.at[7 + i], 1).wait_recv()
    for copy in sent:
        copy.wait_send()
    for copy in own:
        copy.wait()


def exchange(x, m, w1, w2, meta):
    vmem = pl.BlockSpec(memory_space=pltpu.VMEM)
    hbm = pl.BlockSpec(memory_space=pl.ANY)
    return pl.pallas_call(
        exchange_kernel,
        out_shape=(jax.ShapeDtypeStruct((NDEV * UNIQ, DIM), F32), jax.ShapeDtypeStruct((NDEV, 1, META), jnp.int32), jax.ShapeDtypeStruct((2, DIM, FFN), F32)),
        in_specs=[vmem] * 5,
        out_specs=(hbm, vmem, hbm),
        scratch_shapes=[
            pltpu.VMEM((UNIQ, DIM), F32), pltpu.VMEM((2, DIM, FFN), F32), pltpu.VMEM((DIM, FFN), F32), pltpu.VMEM((DIM, FFN), F32),
            pltpu.VMEM((3, QROWS, FFN), F32), pltpu.VMEM((QROWS, FFN), F32),
            pltpu.SemaphoreType.DMA((8, PIECES, 4)), pltpu.SemaphoreType.DMA((8, PIECES)), pltpu.SemaphoreType.DMA((8, 4)), pltpu.SemaphoreType.DMA((8,)),
            pltpu.SemaphoreType.DMA((11,)), pltpu.SemaphoreType.DMA((11,)), pltpu.SemaphoreType.DMA((PIECES + 2,))],
        compiler_params=pltpu.CompilerParams(vmem_limit_bytes=VMEM_LIMIT, collective_id=0, has_side_effects=True),
        name="exchange",
    )(x, m, w1, w2, meta)


def table_kernel(uid_ref, off_ref, rows_hbm, out_hbm, rows, acc, in_sem, out_sem):
    def in_copy(d, half):
        part = pl.ds(d * UNIQ, UNIQ)
        return pltpu.make_async_copy(rows_hbm.at[part, pl.ds(half * 128, 128)], rows.at[half, part], in_sem.at[d, half])

    def out_copy(c, half):
        part = pl.ds(c * CHUNK, CHUNK if c < NCHUNK - 1 else LAST)
        return pltpu.make_async_copy(acc.at[half, part], out_hbm.at[part, pl.ds(half * 128, 128)], out_sem.at[c, half])

    for d in range(NDEV):
        for half in range(2):
            in_copy(d, half).start()

    @pl.loop(0, PADDED // ZERO)
    def _(i):
        part = pl.ds(pl.multiple_of(i * ZERO, ZERO), ZERO)
        for half in range(2):
            acc[half, part] = jnp.zeros((ZERO, 128), F32)

    for d in range(NDEV):
        for half in range(2):
            in_copy(d, half).wait()

    for c in range(NCHUNK):
        for d in range(NDEV):
            first = (off_ref[d * HI + c * CHUNK_HI] + BATCH - 1) // BATCH
            last = (off_ref[d * HI + (c + 1) * CHUNK_HI] + BATCH - 1) // BATCH if c < NCHUNK - 1 else UNIQ // BATCH

            def fetch(b):
                base = pl.multiple_of(d * UNIQ + b * BATCH, BATCH)
                sums = []
                for half in range(2):
                    for k in range(BATCH):
                        sums.append(acc[half, pl.ds(uid_ref[base + k], 1), :] + rows[half, pl.ds(base + k, 1), :])
                return sums

            def put(b, sums):
                base = pl.multiple_of(d * UNIQ + b * BATCH, BATCH)
                for half in range(2):
                    for k in range(BATCH):
                        acc[half, pl.ds(uid_ref[base + k], 1), :] = sums[half * BATCH + k]

            def step(b, sums):
                ahead = fetch(b)
                put(b - 1, sums)
                return ahead

            @pl.when(last > first)
            def _():
                sums = lax.fori_loop(first + 1, last, step, fetch(first))
                put(last - 1, sums)

        for half in range(2):
            out_copy(c, half).start()
    for c in range(NCHUNK):
        for half in range(2):
            out_copy(c, half).wait()


def table(meta, rows):
    return pl.pallas_call(
        table_kernel,
        grid_spec=pltpu.PrefetchScalarGridSpec(
            num_scalar_prefetch=2, grid=(1,),
            in_specs=[pl.BlockSpec(memory_space=pl.ANY)], out_specs=pl.BlockSpec(memory_space=pl.ANY),
            scratch_shapes=[pltpu.VMEM((2, NDEV * UNIQ, 128), F32), pltpu.VMEM((2, PADDED, 128), F32),
                            pltpu.SemaphoreType.DMA((NDEV, 2)), pltpu.SemaphoreType.DMA((NCHUNK, 2))]),
        out_shape=jax.ShapeDtypeStruct((VOCAB, DIM), F32),
        compiler_params=pltpu.CompilerParams(vmem_limit_bytes=VMEM_LIMIT),
        name="table",
    )(meta[:, :UNIQ].reshape(-1), meta[:, UNIQ:].reshape(-1), rows)


def solution(mesh):
    def per_device(tok_ids, grad_out, n_real, embed_table, w_in, w_out):
        meta, msum = dedup(n_real, tok_ids.reshape(1, TOK), grad_out)
        x = jnp.take(embed_table, meta[0, :UNIQ], axis=0, mode='clip')
        all_rows, all_meta, red = exchange(x, msum, w_in, w_out, meta)
        return table(all_meta[:, 0], all_rows), red[0], red[1].T

    return jax.shard_map(per_device, mesh=mesh, in_specs=(P('data'), P('data', None), P('data'), P(), P(), P()), out_specs=(P(), P(), P()), check_vma=False)
```

```python
import functools
import math

import jax
import jax.numpy as jnp
from jax import lax
from jax.experimental import pallas as pl
from jax.experimental.pallas import tpu as pltpu
from jax.sharding import PartitionSpec as P

GELU_A = 0.044715
GELU_C = math.sqrt(2.0 / math.pi)

NDEV = 8
TOK = 4096
VOCAB = 30522
DIM = 256
FFN = 1024
UNIQ = 1024
HI = 128
LO = 256
STEP_TOK = 512
CHUNK_HI = 16
CHUNK = CHUNK_HI * LO
NCHUNK = -(-VOCAB // CHUNK)
LAST = VOCAB - (NCHUNK - 1) * CHUNK
BATCH = 8
PADDED = 30528
ZERO = 192
PIECES = 4
PIECE = UNIQ // PIECES
QROWS = FFN // 4
META = UNIQ + HI

F32 = jnp.float32
BF16 = jnp.bfloat16
VMEM_LIMIT = 62 * 1024 * 1024


def dot(a, b, ca, cb):
    return lax.dot_general(a, b, (((ca,), (cb,)), ((), ())), preferred_element_type=F32)


def iota(shape, axis):
    return lax.broadcasted_iota(jnp.int32, shape, axis)


def dedup_kernel(n_ref, ids_ref, dy_ref, meta_ref, msum_ref):
    ids = ids_ref[...]
    ohi = (iota((HI, TOK), 0) == (ids >> 8)).astype(BF16)
    olo = (iota((LO, TOK), 0) == (ids & 255)).astype(BF16)
    present = (dot(ohi, olo, 1, 1) > 0.5).astype(BF16)
    upper = (iota((LO, LO), 0) < iota((LO, LO), 1)).astype(BF16)
    before = dot(present, upper, 1, 0)
    total = dot(present, jnp.ones((LO, UNIQ), BF16), 1, 0)
    lower = (iota((HI, HI), 1) < iota((HI, HI), 0)).astype(BF16)
    offset = dot(lower, total.astype(BF16), 1, 0)
    rank = before + offset[:, :LO]
    rank_a = jnp.floor(rank * (1.0 / 32.0))
    rank_b = (rank - 32.0 * rank_a).astype(BF16)
    rank_a = rank_a.astype(BF16)

    lane = iota((HI, UNIQ), 1).astype(F32)
    hi_of = jnp.sum(((offset + total) <= lane).astype(F32), axis=0, keepdims=True)
    hot = iota((HI, UNIQ), 0).astype(F32) == hi_of
    k_of = lane[:1] - jnp.sum(jnp.where(hot, offset, 0.0), axis=0, keepdims=True)
    upto = (before + present.astype(F32)).astype(BF16)
    row_of = dot(upto, hot.astype(BF16), 0, 0)
    lo_of = jnp.sum((row_of <= k_of).astype(F32), axis=0, keepdims=True)
    meta_ref[:, :UNIQ] = (hi_of * 256.0 + lo_of).astype(jnp.int32)
    eye = iota((HI, HI), 0) == iota((HI, HI), 1)
    meta_ref[:, UNIQ:] = jnp.sum(jnp.where(eye, offset[:, :HI], 0.0), axis=0, keepdims=True).astype(jnp.int32)

    kept = n_ref[0]
    for b in range(TOK // STEP_TOK):
        cols = slice(b * STEP_TOK, (b + 1) * STEP_TOK)
        mine = ohi[:, cols]
        pos = 32.0 * dot(rank_a, mine, 0, 0) + dot(rank_b, mine, 0, 0)
        slot = jnp.sum(pos * olo[:, cols].astype(F32), axis=0, keepdims=True)
        tok = iota((1, STEP_TOK), 1) + b * STEP_TOK
        slot = jnp.where(tok < kept, slot.astype(jnp.int32), -1)
        pick = (iota((UNIQ, STEP_TOK), 0) == slot).astype(BF16)
        part = dot(pick, dy_ref[cols, :], 1, 0)
        if b == 0:
            msum_ref[...] = part
        else:
            msum_ref[...] += part


def dedup(n_real, ids, dy):
    return pl.pallas_call(
        dedup_kernel,
        out_shape=(jax.ShapeDtypeStruct((1, META), jnp.int32), jax.ShapeDtypeStruct((UNIQ, DIM), F32)),
        in_specs=[pl.BlockSpec(memory_space=pltpu.SMEM), pl.BlockSpec(memory_space=pltpu.VMEM), pl.BlockSpec(memory_space=pltpu.VMEM)],
        out_specs=(pl.BlockSpec(memory_space=pltpu.VMEM), pl.BlockSpec(memory_space=pltpu.VMEM)),
        compiler_params=pltpu.CompilerParams(vmem_limit_bytes=VMEM_LIMIT),
        name="dedup",
    )(n_real, ids, dy)


def exchange_kernel(x_ref, m_ref, w1_ref, w2_ref, meta_ref, rows_ref, meta_out, red_ref,
                    dx, part, pin, chip, rs, fin, row_send, row_recv, meta_send, meta_recv, w_send, w_recv, own_sem):
    me = lax.axis_index('data')
    core, px, py = me % 2, (me // 2) % 2, me // 4

    def dev(r):
        return me + (r & 1) * (1 - 2 * core) + ((r >> 1) & 1) * (2 - 4 * px) + ((r >> 2) & 1) * (4 - 8 * py)

    def remote(src, dst, send, recv, r):
        return pltpu.make_async_remote_copy(src_ref=src, dst_ref=dst, send_sem=send, recv_sem=recv, device_id=(dev(r),), device_id_type=pl.DeviceIdType.MESH)

    barrier = pltpu.get_barrier_semaphore()
    for r in (1, 2, 4, 6):
        pl.semaphore_signal(barrier, inc=1, device_id=(dev(r),), device_id_type=pl.DeviceIdType.MESH)
    pl.semaphore_wait(barrier, 4)

    sent = []

    def rows_at(r, k):
        return rows_ref.at[pl.ds(pl.multiple_of(dev(r) * UNIQ + k * PIECE, PIECE), PIECE)]

    def send_rows(block, k, to, src=None):
        copy = remote(rows_at(block, k) if src is None else src, rows_at(block, k), row_send.at[block, k, to // 2], row_recv.at[block ^ to, k], to)
        copy.start()
        sent.append(copy)

    def got_rows(block, k):
        remote(rows_at(block, k), rows_at(block, k), row_send.at[block, k, 0], row_recv.at[block, k], 1).wait_recv()

    def send_meta(block, to):
        src = meta_ref if block == 0 else meta_out.at[dev(block)]
        copy = remote(src, meta_out.at[dev(block)], meta_send.at[block, to // 2], meta_recv.at[block ^ to], to)
        copy.start()
        sent.append(copy)

    def got_meta(block):
        at = meta_out.at[dev(block)]
        remote(at, at, meta_send.at[block, 0], meta_recv.at[block], 1).wait_recv()

    own = [pltpu.make_async_copy(meta_ref, meta_out.at[me], own_sem.at[PIECES])]
    own[0].start()
    for to in (1, 2, 4, 6):
        send_meta(0, to)

    for k in range(PIECES):
        part_rows = pl.ds(k * PIECE, PIECE)
        x = x_ref[part_rows, :]
        m = m_ref[part_rows, :]
        m_hi = m.astype(BF16)
        m_lo = (m - m_hi.astype(F32)).astype(BF16)
        z = dot(x, w1_ref[...], 1, 0).astype(BF16).astype(F32)
        t = jnp.tanh(GELU_C * (z + GELU_A * z * z * z))
        h = (0.5 * z * (1.0 + t)).astype(BF16)
        slope = 0.5 * (1.0 + t) + 0.5 * z * (1.0 - t * t) * GELU_C * (1.0 + 3.0 * GELU_A * z * z)
        dh = (dot(m_hi, w2_ref[...], 1, 1) + dot(m_lo, w2_ref[...], 1, 1)).astype(BF16).astype(F32)
        dz = (dh * slope).astype(BF16)
        dx[part_rows, :] = m + dot(dz, w1_ref[...], 1, 1)
        for q in range(FFN // DIM):
            cols = slice(q * DIM, (q + 1) * DIM)
            dw1 = dot(x, dz[:, cols], 0, 0)
            part[0, cols] = dw1 if k == 0 else part[0, cols] + dw1
        dw2 = dot(h, m_hi, 0, 0) + dot(h, m_lo, 0, 0)
        part[1] = dw2 if k == 0 else part[1] + dw2
        src = dx.at[part_rows]
        for to in (2, 4, 1):
            send_rows(0, k, to, src)
        copy = pltpu.make_async_copy(src, rows_at(0, k), own_sem.at[k])
        copy.start()
        own.append(copy)

    def w_copy(src, dst, i, to):
        copy = remote(src, dst, w_send.at[i], w_recv.at[i], to)
        copy.start()
        sent.append(copy)

    def quarter(r):
        return pl.ds(pl.multiple_of((dev(r) // 2) * QROWS, QROWS), QROWS)

    w_copy(part.at[1 - core], pin, 0, 1)
    remote(pin, pin, w_send.at[0], w_recv.at[0], 1).wait_recv()
    chip[...] = part[core] + pin[...]
    for i, to in enumerate((2, 4, 6)):
        w_copy(chip.at[quarter(to)], rs.at[i], 1 + i, to)

    for block in (2, 4, 6):
        got_meta(block)
        send_meta(block, 1)

    for k in range(PIECES):
        got_rows(2, k)
        if k < PIECES // 2:
            send_rows(2, k, 4)
        send_rows(2, k, 1)
        got_rows(4, k)
        if k >= PIECES // 2:
            send_rows(4, k, 2)
        send_rows(4, k, 1)

    for i, to in enumerate((2, 4, 6)):
        remote(rs.at[i], rs.at[i], w_send.at[1 + i], w_recv.at[1 + i], to).wait_recv()
    fin[...] = (chip[quarter(0), :] + rs[0]) + (rs[1] + rs[2])

    def red_at(r):
        return red_ref.at[(core + r) % 2, quarter(r)]

    for i, to in enumerate((2, 4, 6)):
        w_copy(fin, red_at(0), 4 + i, to)
    w_copy(fin, red_at(0), 7, 1)
    copy = pltpu.make_async_copy(fin, red_at(0), own_sem.at[PIECES + 1])
    copy.start()
    own.append(copy)

    for k in range(PIECES):
        got_rows(6, k)
        send_rows(6, k, 1)

    for i, block in enumerate((2, 4, 6)):
        remote(red_at(block), red_at(block), w_send.at[4 + i], w_recv.at[4 + i], 1).wait_recv()
        w_copy(red_at(block), red_at(block), 8 + i, 1)

    for block in (1, 3, 5, 7):
        got_meta(block)
        for k in range(PIECES):
            got_rows(block, k)
    for i, block in enumerate((1, 3, 5, 7)):
        remote(red_at(block), red_at(block), w_send.at[7 + i], w_recv.at[7 + i], 1).wait_recv()
    for copy in sent:
        copy.wait_send()
    for copy in own:
        copy.wait()


def exchange(x, m, w1, w2, meta):
    vmem = pl.BlockSpec(memory_space=pltpu.VMEM)
    hbm = pl.BlockSpec(memory_space=pl.ANY)
    return pl.pallas_call(
        exchange_kernel,
        out_shape=(jax.ShapeDtypeStruct((NDEV * UNIQ, DIM), F32), jax.ShapeDtypeStruct((NDEV, 1, META), jnp.int32), jax.ShapeDtypeStruct((2, FFN, DIM), F32)),
        in_specs=[vmem] * 5,
        out_specs=(hbm, vmem, hbm),
        scratch_shapes=[
            pltpu.VMEM((UNIQ, DIM), F32), pltpu.VMEM((2, FFN, DIM), F32), pltpu.VMEM((FFN, DIM), F32), pltpu.VMEM((FFN, DIM), F32),
            pltpu.VMEM((3, QROWS, DIM), F32), pltpu.VMEM((QROWS, DIM), F32),
            pltpu.SemaphoreType.DMA((8, PIECES, 4)), pltpu.SemaphoreType.DMA((8, PIECES)), pltpu.SemaphoreType.DMA((8, 4)), pltpu.SemaphoreType.DMA((8,)),
            pltpu.SemaphoreType.DMA((11,)), pltpu.SemaphoreType.DMA((11,)), pltpu.SemaphoreType.DMA((PIECES + 2,))],
        compiler_params=pltpu.CompilerParams(vmem_limit_bytes=VMEM_LIMIT, collective_id=0, has_side_effects=True),
        name="exchange",
    )(x, m, w1, w2, meta)


def table_kernel(meta_hbm, rows_hbm, red_hbm, out_hbm, w1_hbm, w2_hbm, *scratch):
    meta = scratch[:NDEV]
    rows, acc, red, meta_sem, in_sem, out_sem, red_sem, w_sem = scratch[NDEV:]

    def in_copy(d, half):
        part = pl.ds(d * UNIQ, UNIQ)
        return pltpu.make_async_copy(rows_hbm.at[part, pl.ds(half * 128, 128)], rows.at[half, part], in_sem.at[d, half])

    def out_copy(c, half):
        part = pl.ds(c * CHUNK, CHUNK if c < NCHUNK - 1 else LAST)
        return pltpu.make_async_copy(acc.at[half, part], out_hbm.at[part, pl.ds(half * 128, 128)], out_sem.at[c, half])

    def meta_copy(d):
        return pltpu.make_async_copy(meta_hbm.at[d, 0], meta[d], meta_sem.at[d])

    for d in range(NDEV):
        meta_copy(d).start()
    for d in range(NDEV):
        for half in range(2):
            in_copy(d, half).start()
    red_in = pltpu.make_async_copy(red_hbm, red, red_sem)
    red_in.start()

    @pl.loop(0, PADDED // ZERO)
    def _(i):
        part = pl.ds(pl.multiple_of(i * ZERO, ZERO), ZERO)
        for half in range(2):
            acc[half, part] = jnp.zeros((ZERO, 128), F32)

    for d in range(NDEV):
        meta_copy(d).wait()
        for half in range(2):
            in_copy(d, half).wait()
    red_in.wait()
    w_out = [pltpu.make_async_copy(red.at[1], w2_hbm, w_sem.at[4])]
    for q in range(FFN // DIM):
        w_out.append(pltpu.make_async_copy(red.at[0, pl.ds(q * DIM, DIM)], w1_hbm.at[:, pl.ds(q * DIM, DIM)], w_sem.at[q]))
    for copy in w_out:
        copy.start()

    for c in range(NCHUNK):
        for d in range(NDEV):
            first = (meta[d][UNIQ + c * CHUNK_HI] + BATCH - 1) // BATCH if c else 0
            last = (meta[d][UNIQ + (c + 1) * CHUNK_HI] + BATCH - 1) // BATCH if c < NCHUNK - 1 else UNIQ // BATCH

            def fetch(b):
                base = pl.multiple_of(b * BATCH, BATCH)
                at = [meta[d][base + k] for k in range(BATCH)]
                sums = []
                for k in range(BATCH):
                    for half in range(2):
                        sums.append(acc[half, pl.ds(at[k], 1), :] + rows[half, pl.ds(d * UNIQ + base + k, 1), :])
                return at, sums

            def put(at, sums):
                for k in range(BATCH):
                    for half in range(2):
                        acc[half, pl.ds(at[k], 1), :] = sums[2 * k + half]

            def step(b, carry):
                ahead = fetch(b)
                put(*carry)
                return ahead

            @pl.when(last > first)
            def _():
                put(*lax.fori_loop(first + 1, last, step, fetch(first)))

        for half in range(2):
            out_copy(c, half).start()
    for copy in w_out:
        copy.wait()
    for c in range(NCHUNK):
        for half in range(2):
            out_copy(c, half).wait()


def table(meta, rows, red):
    hbm = pl.BlockSpec(memory_space=pl.ANY)
    return pl.pallas_call(
        table_kernel,
        in_specs=[hbm] * 3, out_specs=(hbm,) * 3,
        scratch_shapes=[pltpu.SMEM((META,), jnp.int32)] * NDEV + [
            pltpu.VMEM((2, NDEV * UNIQ, 128), F32), pltpu.VMEM((2, PADDED, 128), F32), pltpu.VMEM((2, FFN, DIM), F32),
            pltpu.SemaphoreType.DMA((NDEV,)), pltpu.SemaphoreType.DMA((NDEV, 2)), pltpu.SemaphoreType.DMA((NCHUNK, 2)),
            pltpu.SemaphoreType.DMA, pltpu.SemaphoreType.DMA((5,))],
        out_shape=(jax.ShapeDtypeStruct((VOCAB, DIM), F32), jax.ShapeDtypeStruct((DIM, FFN), F32), jax.ShapeDtypeStruct((FFN, DIM), F32)),
        compiler_params=pltpu.CompilerParams(vmem_limit_bytes=VMEM_LIMIT),
        name="table",
    )(meta, rows, red)


def solution(mesh):
    def per_device(tok_ids, grad_out, n_real, embed_table, w_in, w_out):
        meta, msum = dedup(n_real, tok_ids.reshape(1, TOK), grad_out)
        x = jnp.take(embed_table, meta[0, :UNIQ], axis=0, mode='clip')
        all_rows, all_meta, red = exchange(x, msum, w_in, w_out, meta)
        return table(all_meta, all_rows, red)

    return jax.shard_map(per_device, mesh=mesh, in_specs=(P('data'), P('data', None), P('data'), P(), P(), P()), out_specs=(P(), P(), P()), check_vma=False)
```

```python
import functools
import math

import jax
import jax.numpy as jnp
from jax import lax
from jax.experimental import pallas as pl
from jax.experimental.pallas import tpu as pltpu
from jax.sharding import PartitionSpec as P

GELU_A = 0.044715
GELU_C = math.sqrt(2.0 / math.pi)

NDEV = 8
TOK = 4096
VOCAB = 30522
DIM = 256
FFN = 1024
UNIQ = 1024
HI = 128
LO = 256
STEP_TOK = 512
FETCH = UNIQ * STEP_TOK // TOK
LAST_TILE = VOCAB // 8 - 1
CHUNK_HI = 16
CHUNK = CHUNK_HI * LO
NCHUNK = -(-VOCAB // CHUNK)
LAST = VOCAB - (NCHUNK - 1) * CHUNK
BATCH = 8
PADDED = 30528
ZERO = 192
PIECES = 4
PIECE = UNIQ // PIECES
QROWS = FFN // 4
META = UNIQ + HI

F32 = jnp.float32
BF16 = jnp.bfloat16
VMEM_LIMIT = 62 * 1024 * 1024


def dot(a, b, ca, cb):
    return lax.dot_general(a, b, (((ca,), (cb,)), ((), ())), preferred_element_type=F32)


def iota(shape, axis):
    return lax.broadcasted_iota(jnp.int32, shape, axis)


def prepare_kernel(n_ref, ids_ref, dy_ref, tail_ref, e_hbm, meta_ref, msum_ref, x_ref, uid, tiles, uid_sem, tile_sem):
    ids = ids_ref[...]
    ohi = (iota((HI, TOK), 0) == (ids >> 8)).astype(BF16)
    olo = (iota((LO, TOK), 0) == (ids & 255)).astype(BF16)
    present = (dot(ohi, olo, 1, 1) > 0.5).astype(BF16)
    upper = (iota((LO, LO), 0) < iota((LO, LO), 1)).astype(BF16)
    before = dot(present, upper, 1, 0)
    total = dot(present, jnp.ones((LO, UNIQ), BF16), 1, 0)
    lower = (iota((HI, HI), 1) < iota((HI, HI), 0)).astype(BF16)
    offset = dot(lower, total.astype(BF16), 1, 0)

    lane = iota((HI, UNIQ), 1).astype(F32)
    hi_of = jnp.sum(((offset + total) <= lane).astype(F32), axis=0, keepdims=True)
    hot = iota((HI, UNIQ), 0).astype(F32) == hi_of
    k_of = lane[:1] - jnp.sum(jnp.where(hot, offset, 0.0), axis=0, keepdims=True)
    upto = (before + present.astype(F32)).astype(BF16)
    row_of = dot(upto, hot.astype(BF16), 0, 0)
    lo_of = jnp.sum((row_of <= k_of).astype(F32), axis=0, keepdims=True)
    uid_row = (hi_of * 256.0 + lo_of).astype(jnp.int32)
    meta_ref[:, :UNIQ] = uid_row
    eye = iota((HI, HI), 0) == iota((HI, HI), 1)
    meta_ref[:, UNIQ:] = jnp.sum(jnp.where(eye, offset[:, :HI], 0.0), axis=0, keepdims=True).astype(jnp.int32)
    to_smem = pltpu.make_async_copy(meta_ref.at[0], uid, uid_sem)
    to_smem.start()

    rank = before + offset[:, :LO]
    rank_a = jnp.floor(rank * (1.0 / 32.0))
    rank_b = (rank - 32.0 * rank_a).astype(BF16)
    rank_a = rank_a.astype(BF16)
    msum_ref[...] = jnp.zeros((UNIQ, DIM), F32)
    kept = n_ref[0]
    to_smem.wait()

    def step(b, carry):
        for j in range(FETCH):
            at = b * FETCH + j
            tile = jnp.minimum(uid[at] >> 3, LAST_TILE)
            pltpu.make_async_copy(e_hbm.at[pl.ds(pl.multiple_of(tile * 8, 8), 8)], tiles.at[pl.ds(pl.multiple_of(at * 8, 8), 8)], tile_sem).start()
        cols = pl.ds(pl.multiple_of(b * STEP_TOK, STEP_TOK), STEP_TOK)
        mine = ids_ref[:, cols]
        mine_hi = (iota((HI, STEP_TOK), 0) == (mine >> 8)).astype(BF16)
        pos = 32.0 * dot(rank_a, mine_hi, 0, 0) + dot(rank_b, mine_hi, 0, 0)
        slot = jnp.sum(jnp.where(iota((LO, STEP_TOK), 0) == (mine & 255), pos, 0.0), axis=0, keepdims=True)
        tok = iota((1, STEP_TOK), 1) + b * STEP_TOK
        slot = jnp.where(tok < kept, slot.astype(jnp.int32), -1)
        pick = (iota((UNIQ, STEP_TOK), 0) == slot).astype(BF16)
        msum_ref[...] += dot(pick, dy_ref[cols, :], 1, 0)
        return carry

    lax.fori_loop(0, TOK // STEP_TOK, step, 0)
    pltpu.make_async_copy(tiles, tiles, tile_sem).wait()

    uid_col = jnp.broadcast_to(uid_row.astype(F32), (128, UNIQ)).T.astype(jnp.int32)
    place = (uid_col & 7) + 8 * (iota((UNIQ, 128), 0) & 31)
    for g in range(UNIQ // 32):
        want = place[g * 32:(g + 1) * 32]
        lanes = iota((32, 128), 1)
        pick = jnp.concatenate([(want == lanes).astype(BF16), (want == lanes + 128).astype(BF16)], axis=1)
        x_ref[pl.ds(g * 32, 32), :] = dot(pick, tiles[pl.ds(g * 256, 256), :], 1, 0).astype(BF16)

    uid_two = jnp.concatenate([uid_col, uid_col], axis=1)
    x = x_ref[...]
    for r in range(VOCAB - 8 * (LAST_TILE + 1)):
        x = jnp.where(uid_two == 8 * (LAST_TILE + 1) + r, tail_ref[pl.ds(r, 1), :].astype(F32), x.astype(F32)).astype(BF16)
    x_ref[...] = x


def prepare(n_real, ids, dy, table, tail):
    vmem = pl.BlockSpec(memory_space=pltpu.VMEM)
    return pl.pallas_call(
        prepare_kernel,
        out_shape=(jax.ShapeDtypeStruct((1, META), jnp.int32), jax.ShapeDtypeStruct((UNIQ, DIM), F32), jax.ShapeDtypeStruct((UNIQ, DIM), BF16)),
        in_specs=[pl.BlockSpec(memory_space=pltpu.SMEM), vmem, vmem, vmem, pl.BlockSpec(memory_space=pl.ANY)],
        out_specs=(vmem, vmem, vmem),
        scratch_shapes=[pltpu.SMEM((META,), jnp.int32), pltpu.VMEM((8 * UNIQ, DIM), BF16), pltpu.SemaphoreType.DMA, pltpu.SemaphoreType.DMA],
        compiler_params=pltpu.CompilerParams(vmem_limit_bytes=VMEM_LIMIT),
        name="prepare",
    )(n_real, ids, dy, tail, table)


def exchange_kernel(x_ref, m_ref, w1_ref, w2_ref, meta_ref, rows_ref, meta_out, red_ref,
                    dx, part, pin, chip, rs, fin, row_send, row_recv, meta_send, meta_recv, w_send, w_recv, own_sem):
    me = lax.axis_index('data')
    core, px, py = me % 2, (me // 2) % 2, me // 4

    def dev(r):
        return me + (r & 1) * (1 - 2 * core) + ((r >> 1) & 1) * (2 - 4 * px) + ((r >> 2) & 1) * (4 - 8 * py)

    def remote(src, dst, send, recv, r):
        return pltpu.make_async_remote_copy(src_ref=src, dst_ref=dst, send_sem=send, recv_sem=recv, device_id=(dev(r),), device_id_type=pl.DeviceIdType.MESH)

    barrier = pltpu.get_barrier_semaphore()
    for r in (1, 2, 4, 6):
        pl.semaphore_signal(barrier, inc=1, device_id=(dev(r),), device_id_type=pl.DeviceIdType.MESH)
    pl.semaphore_wait(barrier, 4)

    sent = []

    def rows_at(r, k):
        return rows_ref.at[pl.ds(pl.multiple_of(dev(r) * UNIQ + k * PIECE, PIECE), PIECE)]

    def send_rows(block, k, to, src=None):
        copy = remote(rows_at(block, k) if src is None else src, rows_at(block, k), row_send.at[block, k, to // 2], row_recv.at[block ^ to, k], to)
        copy.start()
        sent.append(copy)

    def got_rows(block, k):
        remote(rows_at(block, k), rows_at(block, k), row_send.at[block, k, 0], row_recv.at[block, k], 1).wait_recv()

    def send_meta(block, to):
        src = meta_ref if block == 0 else meta_out.at[dev(block)]
        copy = remote(src, meta_out.at[dev(block)], meta_send.at[block, to // 2], meta_recv.at[block ^ to], to)
        copy.start()
        sent.append(copy)

    def got_meta(block):
        at = meta_out.at[dev(block)]
        remote(at, at, meta_send.at[block, 0], meta_recv.at[block], 1).wait_recv()

    own = [pltpu.make_async_copy(meta_ref, meta_out.at[me], own_sem.at[PIECES])]
    own[0].start()
    for to in (1, 2, 4, 6):
        send_meta(0, to)

    for k in range(PIECES):
        part_rows = pl.ds(k * PIECE, PIECE)
        x = x_ref[part_rows, :]
        m = m_ref[part_rows, :]
        m_hi = m.astype(BF16)
        m_lo = (m - m_hi.astype(F32)).astype(BF16)
        z = dot(x, w1_ref[...], 1, 0).astype(BF16).astype(F32)
        t = jnp.tanh(GELU_C * (z + GELU_A * z * z * z))
        h = (0.5 * z * (1.0 + t)).astype(BF16)
        slope = 0.5 * (1.0 + t) + 0.5 * z * (1.0 - t * t) * GELU_C * (1.0 + 3.0 * GELU_A * z * z)
        dh = (dot(m_hi, w2_ref[...], 1, 1) + dot(m_lo, w2_ref[...], 1, 1)).astype(BF16).astype(F32)
        dz = (dh * slope).astype(BF16)
        dx[part_rows, :] = m + dot(dz, w1_ref[...], 1, 1)
        for q in range(FFN // DIM):
            cols = slice(q * DIM, (q + 1) * DIM)
            dw1 = dot(x, dz[:, cols], 0, 0)
            part[0, cols] = dw1 if k == 0 else part[0, cols] + dw1
        dw2 = dot(h, m_hi, 0, 0) + dot(h, m_lo, 0, 0)
        part[1] = dw2 if k == 0 else part[1] + dw2
        src = dx.at[part_rows]
        for to in (2, 4, 1):
            send_rows(0, k, to, src)
        copy = pltpu.make_async_copy(src, rows_at(0, k), own_sem.at[k])
        copy.start()
        own.append(copy)

    def w_copy(src, dst, i, to):
        copy = remote(src, dst, w_send.at[i], w_recv.at[i], to)
        copy.start()
        sent.append(copy)

    def quarter(r):
        return pl.ds(pl.multiple_of((dev(r) // 2) * QROWS, QROWS), QROWS)

    w_copy(part.at[1 - core], pin, 0, 1)
    remote(pin, pin, w_send.at[0], w_recv.at[0], 1).wait_recv()
    chip[...] = part[core] + pin[...]
    for i, to in enumerate((2, 4, 6)):
        w_copy(chip.at[quarter(to)], rs.at[i], 1 + i, to)

    for block in (2, 4, 6):
        got_meta(block)
        send_meta(block, 1)

    for k in range(PIECES):
        got_rows(2, k)
        if k < PIECES // 2:
            send_rows(2, k, 4)
        send_rows(2, k, 1)
        got_rows(4, k)
        if k >= PIECES // 2:
            send_rows(4, k, 2)
        send_rows(4, k, 1)

    for i, to in enumerate((2, 4, 6)):
        remote(rs.at[i], rs.at[i], w_send.at[1 + i], w_recv.at[1 + i], to).wait_recv()
    fin[...] = (chip[quarter(0), :] + rs[0]) + (rs[1] + rs[2])

    def red_at(r):
        return red_ref.at[(core + r) % 2, quarter(r)]

    for i, to in enumerate((2, 4, 6)):
        w_copy(fin, red_at(0), 4 + i, to)
    w_copy(fin, red_at(0), 7, 1)
    copy = pltpu.make_async_copy(fin, red_at(0), own_sem.at[PIECES + 1])
    copy.start()
    own.append(copy)

    for k in range(PIECES):
        got_rows(6, k)
        send_rows(6, k, 1)

    for i, block in enumerate((2, 4, 6)):
        remote(red_at(block), red_at(block), w_send.at[4 + i], w_recv.at[4 + i], 1).wait_recv()
        w_copy(red_at(block), red_at(block), 8 + i, 1)

    for block in (1, 3, 5, 7):
        got_meta(block)
        for k in range(PIECES):
            got_rows(block, k)
    for i, block in enumerate((1, 3, 5, 7)):
        remote(red_at(block), red_at(block), w_send.at[7 + i], w_recv.at[7 + i], 1).wait_recv()
    for copy in sent:
        copy.wait_send()
    for copy in own:
        copy.wait()


def exchange(x, m, w1, w2, meta):
    vmem = pl.BlockSpec(memory_space=pltpu.VMEM)
    hbm = pl.BlockSpec(memory_space=pl.ANY)
    return pl.pallas_call(
        exchange_kernel,
        out_shape=(jax.ShapeDtypeStruct((NDEV * UNIQ, DIM), F32), jax.ShapeDtypeStruct((NDEV, 1, META), jnp.int32), jax.ShapeDtypeStruct((2, FFN, DIM), F32)),
        in_specs=[vmem] * 5,
        out_specs=(hbm, vmem, hbm),
        scratch_shapes=[
            pltpu.VMEM((UNIQ, DIM), F32), pltpu.VMEM((2, FFN, DIM), F32), pltpu.VMEM((FFN, DIM), F32), pltpu.VMEM((FFN, DIM), F32),
            pltpu.VMEM((3, QROWS, DIM), F32), pltpu.VMEM((QROWS, DIM), F32),
            pltpu.SemaphoreType.DMA((8, PIECES, 4)), pltpu.SemaphoreType.DMA((8, PIECES)), pltpu.SemaphoreType.DMA((8, 4)), pltpu.SemaphoreType.DMA((8,)),
            pltpu.SemaphoreType.DMA((11,)), pltpu.SemaphoreType.DMA((11,)), pltpu.SemaphoreType.DMA((PIECES + 2,))],
        compiler_params=pltpu.CompilerParams(vmem_limit_bytes=VMEM_LIMIT, collective_id=0, has_side_effects=True),
        name="exchange",
    )(x, m, w1, w2, meta)


def table_kernel(meta_hbm, rows_hbm, red_hbm, out_hbm, w1_hbm, w2_hbm, *scratch):
    meta = scratch[:NDEV]
    rows, acc, red, meta_sem, in_sem, out_sem, red_sem, w_sem = scratch[NDEV:]

    def in_copy(d, half):
        part = pl.ds(d * UNIQ, UNIQ)
        return pltpu.make_async_copy(rows_hbm.at[part, pl.ds(half * 128, 128)], rows.at[half, part], in_sem.at[d, half])

    def out_copy(c, half):
        part = pl.ds(c * CHUNK, CHUNK if c < NCHUNK - 1 else LAST)
        return pltpu.make_async_copy(acc.at[half, part], out_hbm.at[part, pl.ds(half * 128, 128)], out_sem.at[c, half])

    def meta_copy(d):
        return pltpu.make_async_copy(meta_hbm.at[d, 0], meta[d], meta_sem.at[d])

    for d in range(NDEV):
        meta_copy(d).start()
    for d in range(NDEV):
        for half in range(2):
            in_copy(d, half).start()
    red_in = pltpu.make_async_copy(red_hbm, red, red_sem)
    red_in.start()

    @pl.loop(0, PADDED // ZERO)
    def _(i):
        part = pl.ds(pl.multiple_of(i * ZERO, ZERO), ZERO)
        for half in range(2):
            acc[half, part] = jnp.zeros((ZERO, 128), F32)

    for d in range(NDEV):
        meta_copy(d).wait()
        for half in range(2):
            in_copy(d, half).wait()
    red_in.wait()
    w_out = [pltpu.make_async_copy(red.at[1], w2_hbm, w_sem.at[4])]
    for q in range(FFN // DIM):
        w_out.append(pltpu.make_async_copy(red.at[0, pl.ds(q * DIM, DIM)], w1_hbm.at[:, pl.ds(q * DIM, DIM)], w_sem.at[q]))
    for copy in w_out:
        copy.start()

    for c in range(NCHUNK):
        for d in range(NDEV):
            first = (meta[d][UNIQ + c * CHUNK_HI] + BATCH - 1) // BATCH if c else 0
            last = (meta[d][UNIQ + (c + 1) * CHUNK_HI] + BATCH - 1) // BATCH if c < NCHUNK - 1 else UNIQ // BATCH

            def read(b):
                return [meta[d][b * BATCH + k] for k in range(BATCH)]

            def fetch(b, at):
                base = pl.multiple_of(b * BATCH, BATCH)
                return [acc[half, pl.ds(at[k], 1), :] + rows[half, pl.ds(d * UNIQ + base + k, 1), :] for k in range(BATCH) for half in range(2)]

            def put(at, sums):
                for k in range(BATCH):
                    for half in range(2):
                        acc[half, pl.ds(at[k], 1), :] = sums[2 * k + half]

            def step(b, carry):
                at_new, at_old, sums_old = carry
                sums_new = fetch(b, at_new)
                at_next = read(b + 1)
                put(at_old, sums_old)
                return at_next, at_new, sums_new

            @pl.when(last > first)
            def _():
                at = read(first)
                _, at, sums = lax.fori_loop(first + 1, last, step, (read(first + 1), at, fetch(first, at)))
                put(at, sums)

        for half in range(2):
            out_copy(c, half).start()
    for copy in w_out:
        copy.wait()
    for c in range(NCHUNK):
        for half in range(2):
            out_copy(c, half).wait()


def table(meta, rows, red):
    hbm = pl.BlockSpec(memory_space=pl.ANY)
    return pl.pallas_call(
        table_kernel,
        in_specs=[hbm] * 3, out_specs=(hbm,) * 3,
        scratch_shapes=[pltpu.SMEM((META,), jnp.int32)] * NDEV + [
            pltpu.VMEM((2, NDEV * UNIQ, 128), F32), pltpu.VMEM((2, PADDED, 128), F32), pltpu.VMEM((2, FFN, DIM), F32),
            pltpu.SemaphoreType.DMA((NDEV,)), pltpu.SemaphoreType.DMA((NDEV, 2)), pltpu.SemaphoreType.DMA((NCHUNK, 2)),
            pltpu.SemaphoreType.DMA, pltpu.SemaphoreType.DMA((5,))],
        out_shape=(jax.ShapeDtypeStruct((VOCAB, DIM), F32), jax.ShapeDtypeStruct((DIM, FFN), F32), jax.ShapeDtypeStruct((FFN, DIM), F32)),
        compiler_params=pltpu.CompilerParams(vmem_limit_bytes=VMEM_LIMIT),
        name="table",
    )(meta, rows, red)


def solution(mesh):
    def per_device(tok_ids, grad_out, n_real, embed_table, w_in, w_out):
        tail = embed_table[8 * (LAST_TILE + 1):].astype(F32)
        meta, msum, x = prepare(n_real, tok_ids.reshape(1, TOK), grad_out, embed_table, tail)
        all_rows, all_meta, red = exchange(x, msum, w_in, w_out, meta)
        return table(all_meta, all_rows, red)

    return jax.shard_map(per_device, mesh=mesh, in_specs=(P('data'), P('data', None), P('data'), P(), P(), P()), out_specs=(P(), P(), P()), check_vma=False)
```

```python
import functools
import math

import jax
import jax.numpy as jnp
from jax import lax
from jax.experimental import pallas as pl
from jax.experimental.pallas import tpu as pltpu
from jax.sharding import PartitionSpec as P

GELU_A = 0.044715
GELU_C = math.sqrt(2.0 / math.pi)

NDEV = 8
TOK = 4096
VOCAB = 30522
DIM = 256
FFN = 1024
UNIQ = 1024
HI = 128
LO = 256
STEP_TOK = 512
FETCH = UNIQ * STEP_TOK // TOK
LAST_TILE = VOCAB // 8 - 1
CHUNK_HI = 16
CHUNK = CHUNK_HI * LO
NCHUNK = -(-VOCAB // CHUNK)
LAST = VOCAB - (NCHUNK - 1) * CHUNK
BATCH = 8
PADDED = 30528
ZERO = 192
PIECES = 4
PIECE = UNIQ // PIECES
EIGHTH = FFN // 8
META = UNIQ + HI

F32 = jnp.float32
BF16 = jnp.bfloat16
VMEM_LIMIT = 62 * 1024 * 1024


def dot(a, b, ca, cb):
    return lax.dot_general(a, b, (((ca,), (cb,)), ((), ())), preferred_element_type=F32)


def iota(shape, axis):
    return lax.broadcasted_iota(jnp.int32, shape, axis)


def prepare_kernel(n_ref, ids_ref, dy_ref, tail_ref, e_hbm, meta_ref, msum_ref, x_ref, uid, tiles, uid_sem, tile_sem):
    ids = ids_ref[...]
    ohi = (iota((HI, TOK), 0) == (ids >> 8)).astype(BF16)
    olo = (iota((LO, TOK), 0) == (ids & 255)).astype(BF16)
    present = (dot(ohi, olo, 1, 1) > 0.5).astype(BF16)
    upper = (iota((LO, LO), 0) < iota((LO, LO), 1)).astype(BF16)
    before = dot(present, upper, 1, 0)
    total = dot(present, jnp.ones((LO, UNIQ), BF16), 1, 0)
    lower = (iota((HI, HI), 1) < iota((HI, HI), 0)).astype(BF16)
    offset = dot(lower, total.astype(BF16), 1, 0)

    lane = iota((HI, UNIQ), 1).astype(F32)
    hi_of = jnp.sum(((offset + total) <= lane).astype(F32), axis=0, keepdims=True)
    hot = iota((HI, UNIQ), 0).astype(F32) == hi_of
    k_of = lane[:1] - jnp.sum(jnp.where(hot, offset, 0.0), axis=0, keepdims=True)
    upto = (before + present.astype(F32)).astype(BF16)
    row_of = dot(upto, hot.astype(BF16), 0, 0)
    lo_of = jnp.sum((row_of <= k_of).astype(F32), axis=0, keepdims=True)
    uid_row = (hi_of * 256.0 + lo_of).astype(jnp.int32)
    meta_ref[:, :UNIQ] = uid_row
    eye = iota((HI, HI), 0) == iota((HI, HI), 1)
    meta_ref[:, UNIQ:] = jnp.sum(jnp.where(eye, offset[:, :HI], 0.0), axis=0, keepdims=True).astype(jnp.int32)
    to_smem = pltpu.make_async_copy(meta_ref.at[0], uid, uid_sem)
    to_smem.start()

    rank = before + offset[:, :LO]
    rank_a = jnp.floor(rank * (1.0 / 32.0))
    rank_b = (rank - 32.0 * rank_a).astype(BF16)
    rank_a = rank_a.astype(BF16)
    msum_ref[...] = jnp.zeros((UNIQ, DIM), F32)
    kept = n_ref[0]
    to_smem.wait()

    def step(b, carry):
        for j in range(FETCH):
            at = b * FETCH + j
            tile = jnp.minimum(uid[at] >> 3, LAST_TILE)
            pltpu.make_async_copy(e_hbm.at[pl.ds(pl.multiple_of(tile * 8, 8), 8)], tiles.at[pl.ds(pl.multiple_of(at * 8, 8), 8)], tile_sem).start()
        cols = pl.ds(pl.multiple_of(b * STEP_TOK, STEP_TOK), STEP_TOK)
        mine = ids_ref[:, cols]
        mine_hi = (iota((HI, STEP_TOK), 0) == (mine >> 8)).astype(BF16)
        pos = 32.0 * dot(rank_a, mine_hi, 0, 0) + dot(rank_b, mine_hi, 0, 0)
        slot = jnp.sum(jnp.where(iota((LO, STEP_TOK), 0) == (mine & 255), pos, 0.0), axis=0, keepdims=True)
        tok = iota((1, STEP_TOK), 1) + b * STEP_TOK
        slot = jnp.where(tok < kept, slot.astype(jnp.int32), -1)
        pick = (iota((UNIQ, STEP_TOK), 0) == slot).astype(BF16)
        msum_ref[...] += dot(pick, dy_ref[cols, :], 1, 0)
        return carry

    lax.fori_loop(0, TOK // STEP_TOK, step, 0)
    pltpu.make_async_copy(tiles, tiles, tile_sem).wait()

    uid_col = jnp.broadcast_to(uid_row.astype(F32), (128, UNIQ)).T.astype(jnp.int32)
    place = (uid_col & 7) + 8 * (iota((UNIQ, 128), 0) & 31)
    for g in range(UNIQ // 32):
        want = place[g * 32:(g + 1) * 32]
        lanes = iota((32, 128), 1)
        pick = jnp.concatenate([(want == lanes).astype(BF16), (want == lanes + 128).astype(BF16)], axis=1)
        x_ref[pl.ds(g * 32, 32), :] = dot(pick, tiles[pl.ds(g * 256, 256), :], 1, 0).astype(BF16)

    uid_two = jnp.concatenate([uid_col, uid_col], axis=1)
    x = x_ref[...]
    for r in range(VOCAB - 8 * (LAST_TILE + 1)):
        x = jnp.where(uid_two == 8 * (LAST_TILE + 1) + r, tail_ref[pl.ds(r, 1), :].astype(F32), x.astype(F32)).astype(BF16)
    x_ref[...] = x


def prepare(n_real, ids, dy, table, tail):
    vmem = pl.BlockSpec(memory_space=pltpu.VMEM)
    return pl.pallas_call(
        prepare_kernel,
        out_shape=(jax.ShapeDtypeStruct((1, META), jnp.int32), jax.ShapeDtypeStruct((UNIQ, DIM), F32), jax.ShapeDtypeStruct((UNIQ, DIM), BF16)),
        in_specs=[pl.BlockSpec(memory_space=pltpu.SMEM), vmem, vmem, vmem, pl.BlockSpec(memory_space=pl.ANY)],
        out_specs=(vmem, vmem, vmem),
        scratch_shapes=[pltpu.SMEM((META,), jnp.int32), pltpu.VMEM((8 * UNIQ, DIM), BF16), pltpu.SemaphoreType.DMA, pltpu.SemaphoreType.DMA],
        compiler_params=pltpu.CompilerParams(vmem_limit_bytes=VMEM_LIMIT),
        name="prepare",
    )(n_real, ids, dy, tail, table)


def exchange_kernel(x_ref, m_ref, w1_ref, w2_ref, meta_ref, rows_ref, meta_out, red_ref,
                    dx, part, pin, chip, first_in, two, second_in, fin, row_send, row_recv, meta_send, meta_recv, w_send, w_recv, own_sem):
    me = lax.axis_index('data')
    core, px, py = me % 2, (me // 2) % 2, me // 4

    def dev(r):
        return me + (r & 1) * (1 - 2 * core) + ((r >> 1) & 1) * (2 - 4 * px) + ((r >> 2) & 1) * (4 - 8 * py)

    def remote(src, dst, send, recv, r):
        return pltpu.make_async_remote_copy(src_ref=src, dst_ref=dst, send_sem=send, recv_sem=recv, device_id=(dev(r),), device_id_type=pl.DeviceIdType.MESH)

    barrier = pltpu.get_barrier_semaphore()
    for r in (1, 2, 4, 6):
        pl.semaphore_signal(barrier, inc=1, device_id=(dev(r),), device_id_type=pl.DeviceIdType.MESH)
    pl.semaphore_wait(barrier, 4)

    sent = []

    def rows_at(r, k):
        return rows_ref.at[pl.ds(pl.multiple_of(dev(r) * UNIQ + k * PIECE, PIECE), PIECE)]

    def send_rows(block, k, to, src=None):
        copy = remote(rows_at(block, k) if src is None else src, rows_at(block, k), row_send.at[block, k, to // 2], row_recv.at[block ^ to, k], to)
        copy.start()
        sent.append(copy)

    def got_rows(block, k):
        remote(rows_at(block, k), rows_at(block, k), row_send.at[block, k, 0], row_recv.at[block, k], 1).wait_recv()

    def send_meta(block, to):
        src = meta_ref if block == 0 else meta_out.at[dev(block)]
        copy = remote(src, meta_out.at[dev(block)], meta_send.at[block, to // 2], meta_recv.at[block ^ to], to)
        copy.start()
        sent.append(copy)

    def got_meta(block):
        at = meta_out.at[dev(block)]
        remote(at, at, meta_send.at[block, 0], meta_recv.at[block], 1).wait_recv()

    own = [pltpu.make_async_copy(meta_ref, meta_out.at[me], own_sem.at[PIECES])]
    own[0].start()
    for to in (1, 2, 4, 6):
        send_meta(0, to)

    def compute(k):
        part_rows = pl.ds(k * PIECE, PIECE)
        x = x_ref[part_rows, :]
        m = m_ref[part_rows, :]
        m_hi = m.astype(BF16)
        m_lo = (m - m_hi.astype(F32)).astype(BF16)
        z = dot(x, w1_ref[...], 1, 0).astype(BF16).astype(F32)
        t = jnp.tanh(GELU_C * (z + GELU_A * z * z * z))
        h = (0.5 * z * (1.0 + t)).astype(BF16)
        slope = 0.5 * (1.0 + t) + 0.5 * z * (1.0 - t * t) * GELU_C * (1.0 + 3.0 * GELU_A * z * z)
        dh = (dot(m_hi, w2_ref[...], 1, 1) + dot(m_lo, w2_ref[...], 1, 1)).astype(BF16).astype(F32)
        dz = (dh * slope).astype(BF16)
        dx[part_rows, :] = m + dot(dz, w1_ref[...], 1, 1)
        for q in range(FFN // DIM):
            cols = slice(q * DIM, (q + 1) * DIM)
            dw1 = dot(x, dz[:, cols], 0, 0)
            part[0, cols] = dw1 if k == 0 else part[0, cols] + dw1
        dw2 = dot(h, m_hi, 0, 0) + dot(h, m_lo, 0, 0)
        part[1] = dw2 if k == 0 else part[1] + dw2
        copy = pltpu.make_async_copy(dx.at[part_rows], rows_at(0, k), own_sem.at[k])
        copy.start()
        own.append(copy)

    def send_own(k, *tos):
        for to in tos:
            send_rows(0, k, to, dx.at[pl.ds(k * PIECE, PIECE)])

    def w_copy(src, dst, i, to):
        copy = remote(src, dst, w_send.at[i], w_recv.at[i], to)
        copy.start()
        sent.append(copy)

    def w_got(dst, i):
        remote(dst, dst, w_send.at[i], w_recv.at[i], 1).wait_recv()

    def forward(k):
        got_rows(2, k)
        if k % 2 == 0:
            send_rows(2, k, 4)
        send_rows(2, k, 1)
        got_rows(4, k)
        if k % 2 == 1:
            send_rows(4, k, 2)
        send_rows(4, k, 1)

    def eighth(half, a, b):
        return pl.ds(pl.multiple_of((half * 4 + a * 2 + b) * EIGHTH, EIGHTH), EIGHTH)

    def pair(half, a):
        return pl.ds(pl.multiple_of((half * 4 + a * 2) * EIGHTH, 2 * EIGHTH), 2 * EIGHTH)

    def red_at(half, flip_x, flip_y, flip_core=0):
        ax = px + flip_x * (1 - 2 * px)
        ay = py + flip_y * (1 - 2 * py)
        a, b = (ax, ay) if half == 0 else (ay, ax)
        return red_ref.at[(core + flip_core) % 2, eighth(half, a, b)]

    compute(0)
    send_own(0, 2, 4, 1)
    compute(1)
    send_own(1, 2, 4, 1)
    compute(2)
    compute(3)
    w_copy(part.at[1 - core], pin, 0, 1)
    send_own(2, 1)
    send_own(3, 1)
    w_got(pin, 0)
    chip[...] = part[core] + pin[...]
    w_copy(chip.at[pair(0, 1 - px)], first_in.at[0], 1, 2)
    w_copy(chip.at[pair(1, 1 - py)], first_in.at[1], 2, 4)
    send_own(2, 2, 4)

    for block in (2, 4, 6):
        got_meta(block)
        send_meta(block, 1)
    forward(0)

    w_got(first_in.at[0], 1)
    two[0] = chip[pair(0, px), :] + first_in[0]
    w_copy(two.at[0, pl.ds(pl.multiple_of((1 - py) * EIGHTH, EIGHTH), EIGHTH)], second_in.at[0], 3, 4)
    w_got(first_in.at[1], 2)
    two[1] = chip[pair(1, py), :] + first_in[1]
    w_copy(two.at[1, pl.ds(pl.multiple_of((1 - px) * EIGHTH, EIGHTH), EIGHTH)], second_in.at[1], 4, 2)
    send_own(3, 2, 4)
    forward(1)

    w_got(second_in.at[0], 3)
    fin[0] = two[0, pl.ds(pl.multiple_of(py * EIGHTH, EIGHTH), EIGHTH), :] + second_in[0]
    w_got(second_in.at[1], 4)
    fin[1] = two[1, pl.ds(pl.multiple_of(px * EIGHTH, EIGHTH), EIGHTH), :] + second_in[1]
    for half in range(2):
        w_copy(fin.at[half], red_at(half, 0, 0), 5 + half, 2)
        w_copy(fin.at[half], red_at(half, 0, 0), 7 + half, 4)
        w_copy(fin.at[half], red_at(half, 0, 0), 11 + half, 1)
        copy = pltpu.make_async_copy(fin.at[half], red_at(half, 0, 0), own_sem.at[PIECES + 1 + half])
        copy.start()
        own.append(copy)
    forward(2)

    w_got(red_at(0, 0, 1), 7)
    w_copy(red_at(0, 0, 1), red_at(0, 0, 1), 9, 2)
    w_copy(red_at(0, 0, 1), red_at(0, 0, 1), 13, 1)
    w_got(red_at(1, 1, 0), 6)
    w_copy(red_at(1, 1, 0), red_at(1, 1, 0), 10, 4)
    w_copy(red_at(1, 1, 0), red_at(1, 1, 0), 14, 1)
    w_got(red_at(0, 1, 0), 5)
    w_copy(red_at(0, 1, 0), red_at(0, 1, 0), 15, 1)
    w_got(red_at(1, 0, 1), 8)
    w_copy(red_at(1, 0, 1), red_at(1, 0, 1), 16, 1)
    forward(3)

    for half in range(2):
        w_got(red_at(half, 1, 1), 9 + half)
        w_copy(red_at(half, 1, 1), red_at(half, 1, 1), 17 + half, 1)
    for k in range(PIECES):
        got_rows(6, k)
        send_rows(6, k, 1)

    for i, (half, fx, fy) in enumerate(((0, 0, 0), (1, 0, 0), (0, 0, 1), (1, 1, 0), (0, 1, 0), (1, 0, 1), (0, 1, 1), (1, 1, 1))):
        w_got(red_at(half, fx, fy, 1), 11 + i)
    for block in (1, 3, 5, 7):
        got_meta(block)
        for k in range(PIECES):
            got_rows(block, k)
    for copy in sent:
        copy.wait_send()
    for copy in own:
        copy.wait()


def exchange(x, m, w1, w2, meta):
    vmem = pl.BlockSpec(memory_space=pltpu.VMEM)
    hbm = pl.BlockSpec(memory_space=pl.ANY)
    return pl.pallas_call(
        exchange_kernel,
        out_shape=(jax.ShapeDtypeStruct((NDEV * UNIQ, DIM), F32), jax.ShapeDtypeStruct((NDEV, 1, META), jnp.int32), jax.ShapeDtypeStruct((2, FFN, DIM), F32)),
        in_specs=[vmem] * 5,
        out_specs=(hbm, vmem, hbm),
        scratch_shapes=[
            pltpu.VMEM((UNIQ, DIM), F32), pltpu.VMEM((2, FFN, DIM), F32), pltpu.VMEM((FFN, DIM), F32), pltpu.VMEM((FFN, DIM), F32),
            pltpu.VMEM((2, 2 * EIGHTH, DIM), F32), pltpu.VMEM((2, 2 * EIGHTH, DIM), F32), pltpu.VMEM((2, EIGHTH, DIM), F32), pltpu.VMEM((2, EIGHTH, DIM), F32),
            pltpu.SemaphoreType.DMA((8, PIECES, 4)), pltpu.SemaphoreType.DMA((8, PIECES)), pltpu.SemaphoreType.DMA((8, 4)), pltpu.SemaphoreType.DMA((8,)),
            pltpu.SemaphoreType.DMA((19,)), pltpu.SemaphoreType.DMA((19,)), pltpu.SemaphoreType.DMA((PIECES + 3,))],
        compiler_params=pltpu.CompilerParams(vmem_limit_bytes=VMEM_LIMIT, collective_id=0, has_side_effects=True),
        name="exchange",
    )(x, m, w1, w2, meta)


def table_kernel(meta_hbm, rows_hbm, red_hbm, out_hbm, w1_hbm, w2_hbm, *scratch):
    meta = scratch[:NDEV]
    rows, acc, red, meta_sem, in_sem, out_sem, red_sem, w_sem = scratch[NDEV:]

    def in_copy(d, half):
        part = pl.ds(d * UNIQ, UNIQ)
        return pltpu.make_async_copy(rows_hbm.at[part, pl.ds(half * 128, 128)], rows.at[half, part], in_sem.at[d, half])

    def out_copy(c, half):
        part = pl.ds(c * CHUNK, CHUNK if c < NCHUNK - 1 else LAST)
        return pltpu.make_async_copy(acc.at[half, part], out_hbm.at[part, pl.ds(half * 128, 128)], out_sem.at[c, half])

    def meta_copy(d):
        return pltpu.make_async_copy(meta_hbm.at[d, 0], meta[d], meta_sem.at[d])

    for d in range(NDEV):
        meta_copy(d).start()
    for d in range(NDEV):
        for half in range(2):
            in_copy(d, half).start()
    red_in = pltpu.make_async_copy(red_hbm, red, red_sem)
    red_in.start()

    @pl.loop(0, PADDED // ZERO)
    def _(i):
        part = pl.ds(pl.multiple_of(i * ZERO, ZERO), ZERO)
        for half in range(2):
            acc[half, part] = jnp.zeros((ZERO, 128), F32)

    for d in range(NDEV):
        meta_copy(d).wait()
        for half in range(2):
            in_copy(d, half).wait()
    red_in.wait()
    w_out = [pltpu.make_async_copy(red.at[1], w2_hbm, w_sem.at[4])]
    for q in range(FFN // DIM):
        w_out.append(pltpu.make_async_copy(red.at[0, pl.ds(q * DIM, DIM)], w1_hbm.at[:, pl.ds(q * DIM, DIM)], w_sem.at[q]))
    for copy in w_out:
        copy.start()

    for c in range(NCHUNK):
        for d in range(NDEV):
            first = (meta[d][UNIQ + c * CHUNK_HI] + BATCH - 1) // BATCH if c else 0
            last = (meta[d][UNIQ + (c + 1) * CHUNK_HI] + BATCH - 1) // BATCH if c < NCHUNK - 1 else UNIQ // BATCH

            def fetch(b):
                base = pl.multiple_of(b * BATCH, BATCH)
                at = [meta[d][base + k] for k in range(BATCH)]
                sums = []
                for k in range(BATCH):
                    for half in range(2):
                        sums.append(acc[half, pl.ds(at[k], 1), :] + rows[half, pl.ds(d * UNIQ + base + k, 1), :])
                return at, sums

            def put(at, sums):
                for k in range(BATCH):
                    for half in range(2):
                        acc[half, pl.ds(at[k], 1), :] = sums[2 * k + half]

            def step(b, carry):
                ahead = fetch(b)
                put(*carry)
                return ahead

            @pl.when(last > first)
            def _():
                put(*lax.fori_loop(first + 1, last, step, fetch(first)))

        for half in range(2):
            out_copy(c, half).start()
    for copy in w_out:
        copy.wait()
    for c in range(NCHUNK):
        for half in range(2):
            out_copy(c, half).wait()


def table(meta, rows, red):
    hbm = pl.BlockSpec(memory_space=pl.ANY)
    return pl.pallas_call(
        table_kernel,
        in_specs=[hbm] * 3, out_specs=(hbm,) * 3,
        scratch_shapes=[pltpu.SMEM((META,), jnp.int32)] * NDEV + [
            pltpu.VMEM((2, NDEV * UNIQ, 128), F32), pltpu.VMEM((2, PADDED, 128), F32), pltpu.VMEM((2, FFN, DIM), F32),
            pltpu.SemaphoreType.DMA((NDEV,)), pltpu.SemaphoreType.DMA((NDEV, 2)), pltpu.SemaphoreType.DMA((NCHUNK, 2)),
            pltpu.SemaphoreType.DMA, pltpu.SemaphoreType.DMA((5,))],
        out_shape=(jax.ShapeDtypeStruct((VOCAB, DIM), F32), jax.ShapeDtypeStruct((DIM, FFN), F32), jax.ShapeDtypeStruct((FFN, DIM), F32)),
        compiler_params=pltpu.CompilerParams(vmem_limit_bytes=VMEM_LIMIT),
        name="table",
    )(meta, rows, red)


def solution(mesh):
    def per_device(tok_ids, grad_out, n_real, embed_table, w_in, w_out):
        tail = embed_table[8 * (LAST_TILE + 1):].astype(F32)
        meta, msum, x = prepare(n_real, tok_ids.reshape(1, TOK), grad_out, embed_table, tail)
        all_rows, all_meta, red = exchange(x, msum, w_in, w_out, meta)
        return table(all_meta, all_rows, red)

    return jax.shard_map(per_device, mesh=mesh, in_specs=(P('data'), P('data', None), P('data'), P(), P(), P()), out_specs=(P(), P(), P()), check_vma=False)
```

```python
import functools
import math

import jax
import jax.numpy as jnp
from jax import lax
from jax.experimental import pallas as pl
from jax.experimental.pallas import tpu as pltpu
from jax.sharding import PartitionSpec as P

GELU_A = 0.044715
GELU_C = math.sqrt(2.0 / math.pi)

NDEV = 8
TOK = 4096
VOCAB = 30522
DIM = 256
FFN = 1024
UNIQ = 1024
HI = 128
LO = 256
STEP_TOK = 512
CHUNK_HI = 16
CHUNK = CHUNK_HI * LO
NCHUNK = -(-VOCAB // CHUNK)
LAST = VOCAB - (NCHUNK - 1) * CHUNK
BATCH = 8
PADDED = 30528
ZERO = 192
PIECES = 4
PIECE = UNIQ // PIECES
ESTEP = 2176
EBLOCK = 128
NESTEP = VOCAB // ESTEP
ETAIL = -(-(VOCAB - NESTEP * ESTEP) // 8) * 8
META = UNIQ + HI

F32 = jnp.float32
BF16 = jnp.bfloat16
VMEM_LIMIT = 62 * 1024 * 1024
VMEM_LIMIT_MAX = 67043328


def dot(a, b, ca, cb):
    return lax.dot_general(a, b, (((ca,), (cb,)), ((), ())), preferred_element_type=F32)


def iota(shape, axis):
    return lax.broadcasted_iota(jnp.int32, shape, axis)


def prepare_kernel(n_ref, ids_ref, dy_ref, meta_ref, msum_ref):
    ids = ids_ref[...]
    ohi = (iota((HI, TOK), 0) == (ids >> 8)).astype(BF16)
    olo = (iota((LO, TOK), 0) == (ids & 255)).astype(BF16)
    present = (dot(ohi, olo, 1, 1) > 0.5).astype(BF16)
    upper = (iota((LO, LO), 0) < iota((LO, LO), 1)).astype(BF16)
    before = dot(present, upper, 1, 0)
    total = dot(present, jnp.ones((LO, UNIQ), BF16), 1, 0)
    lower = (iota((HI, HI), 1) < iota((HI, HI), 0)).astype(BF16)
    offset = dot(lower, total.astype(BF16), 1, 0)

    lane = iota((HI, UNIQ), 1).astype(F32)
    hi_of = jnp.sum(((offset + total) <= lane).astype(F32), axis=0, keepdims=True)
    hot = iota((HI, UNIQ), 0).astype(F32) == hi_of
    k_of = lane[:1] - jnp.sum(jnp.where(hot, offset, 0.0), axis=0, keepdims=True)
    upto = (before + present.astype(F32)).astype(BF16)
    row_of = dot(upto, hot.astype(BF16), 0, 0)
    lo_of = jnp.sum((row_of <= k_of).astype(F32), axis=0, keepdims=True)
    uid_row = (hi_of * 256.0 + lo_of).astype(jnp.int32)
    meta_ref[:, :UNIQ] = uid_row
    eye = iota((HI, HI), 0) == iota((HI, HI), 1)
    meta_ref[:, UNIQ:] = jnp.sum(jnp.where(eye, offset[:, :HI], 0.0), axis=0, keepdims=True).astype(jnp.int32)

    rank = before + offset[:, :LO]
    rank_a = jnp.floor(rank * (1.0 / 32.0))
    rank_b = (rank - 32.0 * rank_a).astype(BF16)
    rank_a = rank_a.astype(BF16)
    msum_ref[...] = jnp.zeros((UNIQ, DIM), F32)
    kept = n_ref[0]

    def step(b, carry):
        cols = pl.ds(pl.multiple_of(b * STEP_TOK, STEP_TOK), STEP_TOK)
        mine = ids_ref[:, cols]
        mine_hi = (iota((HI, STEP_TOK), 0) == (mine >> 8)).astype(BF16)
        pos = 32.0 * dot(rank_a, mine_hi, 0, 0) + dot(rank_b, mine_hi, 0, 0)
        slot = jnp.sum(jnp.where(iota((LO, STEP_TOK), 0) == (mine & 255), pos, 0.0), axis=0, keepdims=True)
        tok = iota((1, STEP_TOK), 1) + b * STEP_TOK
        slot = jnp.where(tok < kept, slot.astype(jnp.int32), -1)
        pick = (iota((UNIQ, STEP_TOK), 0) == slot).astype(BF16)
        msum_ref[...] += dot(pick, dy_ref[cols, :], 1, 0)
        return carry

    lax.fori_loop(0, TOK // STEP_TOK, step, 0)


def prepare(n_real, ids, dy):
    vmem = pl.BlockSpec(memory_space=pltpu.VMEM)
    return pl.pallas_call(
        prepare_kernel,
        out_shape=(jax.ShapeDtypeStruct((1, META), jnp.int32), jax.ShapeDtypeStruct((UNIQ, DIM), F32)),
        in_specs=[pl.BlockSpec(memory_space=pltpu.SMEM), vmem, vmem],
        out_specs=(vmem, vmem),
        compiler_params=pltpu.CompilerParams(vmem_limit_bytes=VMEM_LIMIT),
        name="prepare",
    )(n_real, ids, dy)


def exchange_kernel(m_hbm, w1_ref, w2_ref, meta_ref, tail_ref, e_hbm, rows_ref, meta_out, red_ref,
                    e_wide, stage, all_m, x_wide, dx, part, pin, uid,
                    stage_sem, own_sem, uid_sem, m_send, m_recv, meta_send, meta_recv, dx_send, dx_recv, dx_own, w_send, w_recv):
    me = lax.axis_index('data')
    core, px, py = me % 2, (me // 2) % 2, me // 4

    def dev(r):
        return me + (r % 2) * (1 - 2 * core) + ((r // 2) % 2) * (2 - 4 * px) + (r // 4) * (4 - 8 * py)

    def remote(src, dst, send, recv, r):
        return pltpu.make_async_remote_copy(src_ref=src, dst_ref=dst, send_sem=send, recv_sem=recv, device_id=(dev(r),), device_id_type=pl.DeviceIdType.MESH)

    def piece(k):
        return pl.ds(pl.multiple_of(k * PIECE, PIECE), PIECE)

    def stage_copy(c):
        return pltpu.make_async_copy(e_hbm.at[pl.ds(c * ESTEP, ESTEP)], stage.at[c % 2], stage_sem.at[c % 2])

    own_m = pltpu.make_async_copy(m_hbm, all_m.at[0], own_sem.at[0])
    own_m.start()
    stage_copy(0).start()
    stage_copy(1).start()
    own_meta = pltpu.make_async_copy(meta_ref, meta_out.at[me], own_sem.at[1])
    own_meta.start()

    barrier = pltpu.get_barrier_semaphore()
    for r in (1, 2, 4, 6):
        pl.semaphore_signal(barrier, inc=1, device_id=(dev(r),), device_id_type=pl.DeviceIdType.MESH)
    pl.semaphore_wait(barrier, 4)

    sent = []

    def send_meta(block, to):
        src = meta_ref if block == 0 else meta_out.at[dev(block)]
        copy = remote(src, meta_out.at[dev(block)], meta_send.at[block, to // 2], meta_recv.at[block ^ to], to)
        copy.start()
        sent.append(copy)

    def got_meta(block):
        at = meta_out.at[dev(block)]
        remote(at, at, meta_send.at[block, 0], meta_recv.at[block], 1).wait_recv()

    for to in (2, 4, 6, 1):
        send_meta(0, to)
    for k in range(PIECES):
        for to in (2, 4):
            copy = remote(m_hbm.at[piece(k)], all_m.at[to // 2, piece(k)], m_send.at[to // 2 - 1, k], m_recv.at[to // 2, k], to)
            copy.start()
            sent.append(copy)

    part[...] = jnp.zeros((4, 2, FFN, DIM), F32)

    def widen(block, at, size):
        wide = block.astype(F32)
        for half in range(2):
            e_wide[half, pl.ds(pl.multiple_of(at, 8), size), :] = wide[:, half * 128:(half + 1) * 128]

    for c in range(NESTEP):
        stage_copy(c).wait()

        @pl.loop(0, ESTEP // EBLOCK)
        def _(b):
            at = pl.multiple_of(b * EBLOCK, EBLOCK)
            widen(stage[c % 2, pl.ds(at, EBLOCK), :], c * ESTEP + at, EBLOCK)

        if c + 2 < NESTEP:
            stage_copy(c + 2).start()
    widen(tail_ref[...], NESTEP * ESTEP, ETAIL)

    own_meta.wait()
    for block in (2, 4, 6):
        got_meta(block)
        send_meta(block, 1)
    uid_copies = [pltpu.make_async_copy(meta_out.at[dev(2 * s), 0], uid.at[pl.ds(s * META, META)], uid_sem.at[s]) for s in range(4)]
    for copy in uid_copies:
        copy.start()
    for copy in uid_copies:
        copy.wait()
    own_m.wait()

    def place(i):
        slot = jnp.where(i < PIECES, 0, jnp.where(i < 3 * PIECES, 1 + (i - PIECES) % 2, 3))
        k = jnp.where(i < PIECES, i, jnp.where(i < 3 * PIECES, (i - PIECES) // 2, i - 3 * PIECES))
        return slot, k

    def dx_copies(i, slot, k):
        at = rows_ref.at[pl.ds(pl.multiple_of(dev(2 * slot) * UNIQ + k * PIECE, PIECE), PIECE)]
        return (remote(dx.at[slot, piece(k)], at, dx_send.at[slot, k], dx_recv.at[slot, k], 1),
                pltpu.make_async_copy(dx.at[slot, piece(k)], at, dx_own.at[slot, k]))

    def step(i, carry):
        slot, k = place(i)

        @pl.loop(0, PIECE // 16)
        def _(b):
            base = slot * META + k * PIECE + b * 16
            for j in range(16):
                at = uid[base + j]
                for half in range(2):
                    x_wide[half, pl.ds(b * 16 + j, 1), :] = e_wide[half, pl.ds(at, 1), :]

        here = all_m.at[slot, piece(k)]

        @pl.when(i >= PIECES)
        def _():
            remote(here, here, m_send.at[0, 0], m_recv.at[slot, k], 1).wait_recv()

        @pl.when((slot == 1) & (k % 2 == 0))
        def _():
            remote(here, all_m.at[3, piece(k)], m_send.at[2, k], m_recv.at[3, k], 4).start()

        @pl.when((slot == 2) & (k % 2 == 1))
        def _():
            remote(here, all_m.at[3, piece(k)], m_send.at[2, k], m_recv.at[3, k], 2).start()

        x = jnp.concatenate([x_wide[0], x_wide[1]], axis=1).astype(BF16)
        m = here[...]
        m_hi = m.astype(BF16)
        m_lo = (m - m_hi.astype(F32)).astype(BF16)
        z = dot(x, w1_ref[...], 1, 0).astype(BF16).astype(F32)
        t = jnp.tanh(GELU_C * (z + GELU_A * z * z * z))
        h = (0.5 * z * (1.0 + t)).astype(BF16)
        slope = 0.5 * (1.0 + t) + 0.5 * z * (1.0 - t * t) * GELU_C * (1.0 + 3.0 * GELU_A * z * z)
        dh = (dot(m_hi, w2_ref[...], 1, 1) + dot(m_lo, w2_ref[...], 1, 1)).astype(BF16).astype(F32)
        dz = (dh * slope).astype(BF16)
        dx[slot, piece(k)] = m + dot(dz, w1_ref[...], 1, 1)
        for q in range(FFN // DIM):
            cols = slice(q * DIM, (q + 1) * DIM)
            part[slot, 0, cols] += dot(x, dz[:, cols], 0, 0)
        part[slot, 1] += dot(h, m_hi, 0, 0) + dot(h, m_lo, 0, 0)
        for copy in dx_copies(i, slot, k):
            copy.start()
        return carry

    lax.fori_loop(0, 4 * PIECES, step, 0)

    w_copies = []
    for i in range(2):
        part[0, i] = (part[0, i] + part[1, i]) + (part[2, i] + part[3, i])
        w_copies.append(remote(part.at[0, i], pin.at[i], w_send.at[i], w_recv.at[i], 1))
        w_copies[i].start()
    for i in range(2):
        w_copies[i].wait()
        red_ref[i] = part[0, i] + pin[i]

    @pl.loop(0, 4 * PIECES)
    def _(i):
        slot, k = place(i)
        away, near = dx_copies(i, slot, k)
        away.wait_send()
        near.wait()
        at = rows_ref.at[pl.ds(pl.multiple_of(dev(2 * slot + 1) * UNIQ + k * PIECE, PIECE), PIECE)]
        remote(at, at, dx_send.at[slot, k], dx_recv.at[slot, k], 1).wait_recv()

    for k in range(PIECES):
        here = all_m.at[1 + k % 2, piece(k)]
        remote(here, all_m.at[3, piece(k)], m_send.at[2, k], m_recv.at[3, k], 4 - 2 * (k % 2)).wait_send()
    for block in (1, 3, 5, 7):
        got_meta(block)
    for copy in sent:
        copy.wait_send()


def exchange(m, w1, w2, meta, tail, table):
    vmem = pl.BlockSpec(memory_space=pltpu.VMEM)
    hbm = pl.BlockSpec(memory_space=pl.ANY)
    dma = pltpu.SemaphoreType.DMA
    return pl.pallas_call(
        exchange_kernel,
        out_shape=(jax.ShapeDtypeStruct((NDEV * UNIQ, DIM), F32), jax.ShapeDtypeStruct((NDEV, 1, META), jnp.int32), jax.ShapeDtypeStruct((2, FFN, DIM), F32)),
        in_specs=[hbm, vmem, vmem, vmem, vmem, hbm],
        out_specs=(hbm, vmem, vmem),
        scratch_shapes=[
            pltpu.VMEM((2, NESTEP * ESTEP + ETAIL, 128), F32), pltpu.VMEM((2, ESTEP, DIM), BF16), pltpu.VMEM((4, UNIQ, DIM), F32),
            pltpu.VMEM((2, PIECE, 128), F32), pltpu.VMEM((4, UNIQ, DIM), F32), pltpu.VMEM((4, 2, FFN, DIM), F32), pltpu.VMEM((2, FFN, DIM), F32),
            pltpu.SMEM((4 * META,), jnp.int32),
            dma((2,)), dma((2,)), dma((4,)), dma((3, PIECES)), dma((4, PIECES)), dma((8, 4)), dma((8,)),
            dma((4, PIECES)), dma((4, PIECES)), dma((4, PIECES)), dma((2,)), dma((2,))],
        compiler_params=pltpu.CompilerParams(vmem_limit_bytes=VMEM_LIMIT_MAX, collective_id=0, has_side_effects=True),
        name="exchange",
    )(m, w1, w2, meta, tail, table)


def table_kernel(meta_hbm, rows_hbm, red_hbm, out_hbm, w1_hbm, w2_hbm, *scratch):
    meta = scratch[:NDEV]
    rows, acc, red, meta_sem, in_sem, out_sem, red_sem, w_sem = scratch[NDEV:]

    def in_copy(d, half):
        part = pl.ds(d * UNIQ, UNIQ)
        return pltpu.make_async_copy(rows_hbm.at[part, pl.ds(half * 128, 128)], rows.at[half, part], in_sem.at[d, half])

    def out_copy(c, half):
        part = pl.ds(c * CHUNK, CHUNK if c < NCHUNK - 1 else LAST)
        return pltpu.make_async_copy(acc.at[half, part], out_hbm.at[part, pl.ds(half * 128, 128)], out_sem.at[c, half])

    def meta_copy(d):
        return pltpu.make_async_copy(meta_hbm.at[d, 0], meta[d], meta_sem.at[d])

    for d in range(NDEV):
        meta_copy(d).start()
    for d in range(NDEV):
        for half in range(2):
            in_copy(d, half).start()
    red_in = pltpu.make_async_copy(red_hbm, red, red_sem)
    red_in.start()

    @pl.loop(0, PADDED // ZERO)
    def _(i):
        part = pl.ds(pl.multiple_of(i * ZERO, ZERO), ZERO)
        for half in range(2):
            acc[half, part] = jnp.zeros((ZERO, 128), F32)

    for d in range(NDEV):
        meta_copy(d).wait()
        for half in range(2):
            in_copy(d, half).wait()
    red_in.wait()
    w_out = [pltpu.make_async_copy(red.at[1], w2_hbm, w_sem.at[4])]
    for q in range(FFN // DIM):
        w_out.append(pltpu.make_async_copy(red.at[0, pl.ds(q * DIM, DIM)], w1_hbm.at[:, pl.ds(q * DIM, DIM)], w_sem.at[q]))
    for copy in w_out:
        copy.start()

    for c in range(NCHUNK):
        for d in range(NDEV):
            first = (meta[d][UNIQ + c * CHUNK_HI] + BATCH - 1) // BATCH if c else 0
            last = (meta[d][UNIQ + (c + 1) * CHUNK_HI] + BATCH - 1) // BATCH if c < NCHUNK - 1 else UNIQ // BATCH

            def fetch(b):
                base = pl.multiple_of(b * BATCH, BATCH)
                at = [meta[d][base + k] for k in range(BATCH)]
                sums = []
                for k in range(BATCH):
                    for half in range(2):
                        sums.append(acc[half, pl.ds(at[k], 1), :] + rows[half, pl.ds(d * UNIQ + base + k, 1), :])
                return at, sums

            def put(at, sums):
                for k in range(BATCH):
                    for half in range(2):
                        acc[half, pl.ds(at[k], 1), :] = sums[2 * k + half]

            def step(b, carry):
                ahead = fetch(b)
                put(*carry)
                return ahead

            @pl.when(last > first)
            def _():
                put(*lax.fori_loop(first + 1, last, step, fetch(first)))

        for half in range(2):
            out_copy(c, half).start()
    for copy in w_out:
        copy.wait()
    for c in range(NCHUNK):
        for half in range(2):
            out_copy(c, half).wait()


def table(meta, rows, red):
    hbm = pl.BlockSpec(memory_space=pl.ANY)
    return pl.pallas_call(
        table_kernel,
        in_specs=[hbm] * 3, out_specs=(hbm,) * 3,
        scratch_shapes=[pltpu.SMEM((META,), jnp.int32)] * NDEV + [
            pltpu.VMEM((2, NDEV * UNIQ, 128), F32), pltpu.VMEM((2, PADDED, 128), F32), pltpu.VMEM((2, FFN, DIM), F32),
            pltpu.SemaphoreType.DMA((NDEV,)), pltpu.SemaphoreType.DMA((NDEV, 2)), pltpu.SemaphoreType.DMA((NCHUNK, 2)),
            pltpu.SemaphoreType.DMA, pltpu.SemaphoreType.DMA((5,))],
        out_shape=(jax.ShapeDtypeStruct((VOCAB, DIM), F32), jax.ShapeDtypeStruct((DIM, FFN), F32), jax.ShapeDtypeStruct((FFN, DIM), F32)),
        compiler_params=pltpu.CompilerParams(vmem_limit_bytes=VMEM_LIMIT),
        name="table",
    )(meta, rows, red)


def solution(mesh):
    def per_device(tok_ids, grad_out, n_real, embed_table, w_in, w_out):
        meta, msum = prepare(n_real, tok_ids.reshape(1, TOK), grad_out)
        left = embed_table[NESTEP * ESTEP:].astype(F32)
        left = jnp.pad(left, ((0, ETAIL - left.shape[0]), (0, 0)))
        all_rows, all_meta, red = exchange(msum, w_in, w_out, meta, left, embed_table)
        return table(all_meta, all_rows, red)

    return jax.shard_map(per_device, mesh=mesh, in_specs=(P('data'), P('data', None), P('data'), P(), P(), P()), out_specs=(P(), P(), P()), check_vma=False)
```
